32 devices in a mesh: seq: 8 (over z, x), exp: 4 (over y, core).
Axes of the slice: x: 2, y: 2, z: 4, core: 2. Of those that a mesh axis runs over, the one named last changes fastest.
Arguments:
- tokens: bfloat16 [4, 1024, 4096], P('exp', 'seq'), may hold values from -6 to 6
- out_grad: bfloat16 [4, 1024, 4096], P('exp', 'seq'), may hold values from -0.59765625 to 0.59765625
- router_weight: bfloat16 [4096, 32], replicated, may hold values from -8 to 8
- gate_weight: bfloat16 [32, 4096, 768], P(('seq', 'exp')), may hold values from -0.09375 to 0.09375
- up_weight: bfloat16 [32, 4096, 768], P(('seq', 'exp')), may hold values from -0.09375 to 0.09375
- down_weight: bfloat16 [32, 768, 4096], P(('seq', 'exp')), may hold values from -0.21875 to 0.21875
- saved_gate: bfloat16 [32, 2048, 768], P(('seq', 'exp')), may hold values from -6 to 6
- saved_up: bfloat16 [32, 2048, 768], P(('seq', 'exp')), may hold values from -6 to 6
- expert_ids: int32 [4, 1024, 8], P('exp', 'seq'), may hold values from 0 to 31, as said below
- aux_weight: float32 [1], replicated, may hold values from 2 to 6
Outputs:
- token_grad: bfloat16 [4, 1024, 4096], P('exp', 'seq')
- combine_grad: float32 [4, 1024, 8], P('exp', 'seq')
- router_grad: float32 [4096, 32], P(('seq', 'exp'))
The draws below stay inside these ranges and needn't reach their ends.
Inputs may be any that keep to these rules, and one draw needn't show every extreme that they name: `expert_ids`: among the rows of one device (128 tokens) each expert is named at most 64 times, and some expert exactly 64 times; a token's 8 experts differ.
All inputs are finite; a program needn't handle non-finite values.
Results may differ from the reference program's by a relative error of at most 0.013.
Values may be sent and summed in bfloat16 or wider, within the bound.
A program may use at most 192 MiB of HBM per device.

```python
import math
import jax
import jax.numpy as jnp
from jax import lax

D = 4096
FF = 768
TOP = 8
TOK_DEV = 128
EXPERTS = 32
CAP = 64
SLOTS = 2048
GROUPS = 4
GROUP_TOK = 1024
N_SEQ = 8
N_EXP = 4


def draw_router_weight(key, part):
    drawn = jax.random.normal(key, (D, EXPERTS), jnp.float32) / math.sqrt(D)
    return jnp.clip(drawn, -8.0, 8.0).astype(jnp.bfloat16)


def draw_expert_ids(key, part):
    block_count = GROUPS * (GROUP_TOK // TOK_DEV)
    block_keys = jax.random.split(jax.random.fold_in(key, 11), block_count)
    full_count = TOK_DEV * TOP // CAP

    def one_block(block_key):
        order = jax.random.permutation(block_key, EXPERTS).astype(jnp.int32)
        picked = order[:full_count]
        items = jnp.repeat(picked, CAP, total_repeat_length=TOK_DEV * TOP)
        return items.reshape(TOP, TOK_DEV).T
    drawn = jax.vmap(one_block)(block_keys)
    return drawn.reshape(GROUPS, GROUP_TOK, TOP).astype(jnp.int32)


def shard_levels(rng, dims, pieces, low, largest):
    level, own = 1.0, jax.random.fold_in(rng, 6)
    for dim, parts in pieces:
        draws = jnp.exp(jax.random.uniform(jax.random.fold_in(own, dim), (parts,), jnp.float32, low / len(pieces), largest / len(pieces)))
        level = level * jnp.repeat(draws, dims[dim] // parts).reshape([-1 if axis == dim else 1 for axis in range(len(dims))])
    return level


def noise(stream_key, extent, deviation, most, cuts=(), kind=jnp.bfloat16):
    entries = jax.random.normal(stream_key, extent, jnp.float32) * deviation
    if len(cuts) > 0:
        entries = shard_levels(stream_key, extent, cuts, -0.22, 0.18) * entries
    return jnp.clip(entries, min=-most, max=most).astype(kind)


def setup_inputs(seed: int = 0) -> dict:
    seeds = jax.random.split(jax.random.key(seed), 11)
    return {
        "tokens": noise(seeds[0], (GROUPS, GROUP_TOK, D), 1.0, 6.0, ((0, 4), (1, 8))),
        "out_grad": noise(seeds[1], (GROUPS, GROUP_TOK, D), 0.1, 0.59765625, ((0, 4), (1, 8))),
        "router_weight": draw_router_weight(jax.random.fold_in(seeds[10], 71), 0),
        "gate_weight": noise(seeds[3], (EXPERTS, D, FF), D ** -0.5, 0.09375, ((0, 32),)),
        "up_weight": noise(seeds[4], (EXPERTS, D, FF), D ** -0.5, 0.09375, ((0, 32),)),
        "down_weight": noise(seeds[5], (EXPERTS, FF, D), FF ** -0.5, 0.21875, ((0, 32),)),
        "saved_gate": noise(seeds[6], (EXPERTS, SLOTS, FF), 1.0, 6.0, ((0, 32),)),
        "saved_up": noise(seeds[7], (EXPERTS, SLOTS, FF), 1.0, 6.0, ((0, 32),)),
        "expert_ids": draw_expert_ids(jax.random.fold_in(seeds[10], 71), 0),
        "aux_weight": jnp.clip(jax.random.uniform(seeds[9], (1,), jnp.float32, 2.0, 6.0), 2.0, 6.0),
    }


def expert_backward(grad_rows, gate_rows, w_gate, w_up, w_down, pre_gate, pre_up):
    upstream = jnp.einsum("rd,fd->rf", grad_rows, w_down, preferred_element_type=jnp.float32)
    first = pre_gate.astype(jnp.float32)
    second = pre_up.astype(jnp.float32)
    gate_sig = jax.nn.sigmoid(first)
    gate_act = first * gate_sig
    hidden = gate_act * second
    slot_combine = jnp.sum(upstream * hidden, axis=-1).astype(jnp.bfloat16)
    scaled = gate_rows.astype(jnp.float32)[:, None] * upstream
    grad_first = (scaled * second * gate_sig * (1.0 + first * (1.0 - gate_sig))).astype(jnp.bfloat16)
    grad_second = (scaled * gate_act).astype(jnp.bfloat16)
    back_rows = jnp.einsum("rf,df->rd", grad_first, w_gate, preferred_element_type=jnp.float32)
    back_rows = back_rows + jnp.einsum("rf,df->rd", grad_second, w_up, preferred_element_type=jnp.float32)
    return back_rows.astype(jnp.bfloat16), slot_combine


def reference(tokens, out_grad, router_weight, gate_weight, up_weight, down_weight, saved_gate, saved_up, expert_ids, aux_weight):
    groups, group_tok, model_width = tokens.shape
    experts = router_weight.shape[1]
    slot_count = saved_gate.shape[1]
    capacity = slot_count // (N_SEQ * N_EXP)
    total_rows = groups * group_tok
    inputs = tokens.reshape(total_rows, model_width)
    upstream_grad = out_grad.reshape(total_rows, model_width)
    chosen_ids = expert_ids.reshape(total_rows, TOP)
    logits = jnp.dot(inputs, router_weight, preferred_element_type=jnp.float32)
    router_probs = jax.nn.softmax(logits, axis=-1)
    chosen = jnp.take_along_axis(router_probs, chosen_ids, axis=1)
    chosen_sum = jnp.sum(chosen, axis=1, keepdims=True)
    gate_vals = chosen / chosen_sum
    onehot = (chosen_ids[:, :, None] == jnp.arange(experts, dtype=jnp.int32)[None, None, :]).astype(jnp.int32)
    blocks = total_rows // TOK_DEV
    per_block = onehot.reshape(blocks, TOK_DEV * TOP, experts)
    rank_before = jnp.cumsum(per_block, axis=1) - per_block
    slot_pos = jnp.sum(rank_before * per_block, axis=-1).reshape(total_rows, TOP)
    row_index = jnp.arange(total_rows, dtype=jnp.int32)
    group_of = row_index // group_tok
    within = row_index % group_tok
    source = (within // TOK_DEV) * N_EXP + group_of
    slot_index = (chosen_ids * slot_count + source[:, None] * capacity + slot_pos).astype(jnp.int32).reshape(-1)
    slot_token = jnp.full((experts * slot_count,), total_rows, jnp.int32).at[slot_index].set(jnp.repeat(row_index, TOP))
    gate_slots = jnp.zeros((experts * slot_count,), jnp.bfloat16).at[slot_index].set(gate_vals.reshape(-1).astype(jnp.bfloat16))
    grad_padded = jnp.concatenate([upstream_grad, jnp.zeros((1, model_width), jnp.bfloat16)], axis=0)

    def one_expert(accumulated, expert):
        own_rows = lax.dynamic_slice_in_dim(slot_token, expert * slot_count, slot_count)
        own_gates = lax.dynamic_slice_in_dim(gate_slots, expert * slot_count, slot_count)
        back_rows, slot_combine = expert_backward(grad_padded[own_rows], own_gates, gate_weight[expert], up_weight[expert], down_weight[expert], saved_gate[expert], saved_up[expert])
        accumulated = accumulated.at[own_rows].add(back_rows.astype(jnp.float32))
        return accumulated, slot_combine

    expert_sum, all_combine = lax.scan(one_expert, jnp.zeros((total_rows + 1, model_width), jnp.float32), jnp.arange(experts, dtype=jnp.int32))
    combine_grad = all_combine.reshape(-1)[slot_index].reshape(total_rows, TOP).astype(jnp.float32)
    prob_sel = (combine_grad - jnp.sum(gate_vals * combine_grad, axis=1, keepdims=True)) / chosen_sum
    prob_grad = jnp.einsum("tk,tke->te", prob_sel, onehot.astype(jnp.float32))
    chosen_count = jnp.sum(onehot, axis=1).astype(jnp.float32)
    seq_counts = jnp.sum(chosen_count.reshape(groups, group_tok, experts), axis=1)
    fraction = experts * seq_counts / (TOP * group_tok)
    prob_grad = prob_grad + aux_weight[0] * jnp.repeat(fraction, group_tok, axis=0)
    dlogits = router_probs * (prob_grad - jnp.sum(router_probs * prob_grad, axis=1, keepdims=True))
    logit_grad = dlogits.astype(jnp.bfloat16)
    token_grad = expert_sum[:total_rows] + jnp.einsum("te,de->td", logit_grad, router_weight, preferred_element_type=jnp.float32)
    router_grad = jnp.einsum("td,te->de", inputs, logit_grad, preferred_element_type=jnp.float32)
    return (token_grad.astype(jnp.bfloat16).reshape(groups, group_tok, model_width), combine_grad.reshape(groups, group_tok, TOP), router_grad)
```

```python
import jax
import jax.numpy as jnp
from jax import lax
from jax.experimental import pallas as pl
from jax.experimental.pallas import tpu as pltpu
from jax.sharding import PartitionSpec as P


def expert_backward(grad_rows, gate_rows, w_gate, w_up, w_down, pre_gate, pre_up):
    upstream = jnp.einsum("rd,fd->rf", grad_rows, w_down, preferred_element_type=jnp.float32)
    first = pre_gate.astype(jnp.float32)
    second = pre_up.astype(jnp.float32)
    gate_sig = jax.nn.sigmoid(first)
    gate_act = first * gate_sig
    hidden = gate_act * second
    slot_combine = jnp.sum(upstream * hidden, axis=-1).astype(jnp.bfloat16)
    scaled = gate_rows.astype(jnp.float32)[:, None] * upstream
    grad_first = (scaled * second * gate_sig * (1.0 + first * (1.0 - gate_sig))).astype(
        jnp.bfloat16
    )
    grad_second = (scaled * gate_act).astype(jnp.bfloat16)
    back_rows = jnp.einsum("rf,df->rd", grad_first, w_gate, preferred_element_type=jnp.float32)
    back_rows = back_rows + jnp.einsum(
        "rf,df->rd", grad_second, w_up, preferred_element_type=jnp.float32
    )
    return (back_rows.astype(jnp.bfloat16), slot_combine)


def shards(
    tokens,
    out_grad,
    router_weight,
    gate_weight,
    up_weight,
    down_weight,
    saved_gate,
    saved_up,
    expert_ids,
    aux_weight,
):
    seq_size = lax.axis_size("seq")
    exp_size = lax.axis_size("exp")
    devices = seq_size * exp_size
    inputs = tokens[0]
    upstream_grad = out_grad[0]
    chosen_ids = expert_ids[0]
    tok_rows, top_count = chosen_ids.shape
    model_width = inputs.shape[1]
    experts = router_weight.shape[1]
    capacity = saved_gate.shape[1] // devices
    logits = jnp.dot(inputs, router_weight, preferred_element_type=jnp.float32)
    router_probs = jax.nn.softmax(logits, axis=-1)
    chosen = jnp.take_along_axis(router_probs, chosen_ids, axis=1)
    chosen_sum = jnp.sum(chosen, axis=1, keepdims=True)
    gate_vals = chosen / chosen_sum
    onehot = (
        chosen_ids.reshape(-1)[:, None] == jnp.arange(experts, dtype=jnp.int32)[None, :]
    ).astype(jnp.int32)
    rank_before = jnp.cumsum(onehot, axis=0) - onehot
    slot_pos = jnp.sum(rank_before * onehot, axis=1)
    slot_index = chosen_ids.reshape(-1) * capacity + slot_pos
    token_order = jnp.arange(tok_rows * top_count, dtype=jnp.int32) // top_count
    slot_token = (
        jnp.full((experts * capacity,), tok_rows, jnp.int32).at[slot_index].set(token_order)
    )
    grad_padded = jnp.concatenate(
        [upstream_grad, jnp.zeros((1, model_width), jnp.bfloat16)], axis=0
    )
    grad_slots = grad_padded[slot_token]
    gate_slots = (
        jnp.zeros((experts * capacity,), jnp.bfloat16)
        .at[slot_index]
        .set(gate_vals.reshape(-1).astype(jnp.bfloat16))
    )
    chosen_count = jnp.sum(onehot.reshape(tok_rows, top_count, experts), axis=1).astype(jnp.float32)
    local_counts = jnp.sum(chosen_count, axis=0)
    seq_counts = lax.psum(local_counts, "seq")
    recv_grad, recv_gate = (
        lax.all_to_all(
            grad_slots.reshape(experts, 1, capacity, model_width),
            ("seq", "exp"),
            split_axis=0,
            concat_axis=1,
            tiled=True,
        ),
        lax.all_to_all(
            gate_slots.reshape(experts, 1, capacity),
            ("seq", "exp"),
            split_axis=0,
            concat_axis=1,
            tiled=True,
        ),
    )
    back_rows, slot_combine = expert_backward(
        recv_grad.reshape(-1, model_width),
        recv_gate.reshape(-1),
        gate_weight[0],
        up_weight[0],
        down_weight[0],
        saved_gate[0],
        saved_up[0],
    )
    returned, combine_back = (
        lax.all_to_all(
            back_rows.reshape(1, devices, capacity, model_width),
            ("seq", "exp"),
            split_axis=1,
            concat_axis=0,
            tiled=True,
        ),
        lax.all_to_all(
            slot_combine.reshape(1, devices, capacity),
            ("seq", "exp"),
            split_axis=1,
            concat_axis=0,
            tiled=True,
        ),
    )
    returned_rows = returned.reshape(experts * capacity, model_width)
    expert_sum = jnp.sum(
        returned_rows[slot_index].reshape(tok_rows, top_count, model_width).astype(jnp.float32),
        axis=1,
    )
    combine_grad = (
        combine_back.reshape(-1)[slot_index].reshape(tok_rows, top_count).astype(jnp.float32)
    )
    prob_sel = (
        combine_grad - jnp.sum(gate_vals * combine_grad, axis=1, keepdims=True)
    ) / chosen_sum
    prob_grad = jnp.einsum(
        "tk,tke->te", prob_sel, onehot.reshape(tok_rows, top_count, experts).astype(jnp.float32)
    )
    fraction = experts * seq_counts / (top_count * tok_rows * seq_size)
    prob_grad = prob_grad + aux_weight[0] * fraction[None, :]
    dlogits = router_probs * (prob_grad - jnp.sum(router_probs * prob_grad, axis=1, keepdims=True))
    logit_grad = dlogits.astype(jnp.bfloat16)
    token_grad = expert_sum + jnp.einsum(
        "te,de->td", logit_grad, router_weight, preferred_element_type=jnp.float32
    )
    router_grad = lax.psum_scatter(
        jnp.einsum("td,te->de", inputs, logit_grad, preferred_element_type=jnp.float32),
        ("seq", "exp"),
        scatter_dimension=0,
        tiled=True,
    )
    return (token_grad.astype(jnp.bfloat16)[None], combine_grad[None], router_grad)

MESH = pl.DeviceIdType.MESH
CHUNK_ORDERS = (
    (False, False),
    (False, True),
    (True, False),
    (False, True),
    (False, False),
    (True, True),
    (False, True),
    (False, False),
)
CHUNKS = len(CHUNK_ORDERS)
LEVELS = 4
BLOCKS = 4 * LEVELS
STEP_WIDTH = 0.75


def place_of():
    seq, exp = lax.axis_index("seq"), lax.axis_index("exp")
    return seq // 2, seq % 2, exp // 2, exp % 2


def nearest(z, k):
    table = ((0, 1, 2, 3), (1, 2, 0, 3), (2, 1, 3, 0), (3, 2, 1, 0))
    value = jnp.int32(table[3][k])
    for level in (2, 1, 0):
        value = jnp.where(z == level, jnp.int32(table[level][k]), value)
    return value


def planar(first, second, swap):
    return (second, first) if swap else (first, second)


class Copies:
    def __init__(self, swap):
        self.z, self.x, self.y, self.c = place_of()
        self.swap = swap
        self.p, self.q = planar(self.x, self.y, swap)

    def block(self, z, p, q):
        x, y = planar(p, q, self.swap)
        return (z * 2 + x) * 2 + y

    def device(self, z, p, q):
        x, y = planar(p, q, self.swap)
        return z * 2 + x, y * 2 + self.c

    def remote(self, src, dst, send, recv, z, p, q):
        return pltpu.make_async_remote_copy(
            src_ref=src,
            dst_ref=dst,
            send_sem=send,
            recv_sem=recv,
            device_id=self.device(z, p, q),
            device_id_type=MESH,
        )


def sibling_copy(src, dst, send, recv):
    z, x, y, c = place_of()
    return pltpu.make_async_remote_copy(
        src_ref=src,
        dst_ref=dst,
        send_sem=send,
        recv_sem=recv,
        device_id=(z * 2 + x, y * 2 + 1 - c),
        device_id_type=MESH,
    )


def gather_names(chunk):
    if CHUNK_ORDERS[chunk][0]:
        middle = [("Z", k) for k in (1, 2, 3)] + [("P", k) for k in range(4)]
    else:
        middle = [("P", 0)] + [("Z", k) for k in (1, 2, 3)] + [("Y", k) for k in (1, 2, 3)]
    return [("own", 0)] + middle + [("Q", 0), ("near", 0), ("far", 0)]


def pipelined(names):
    timed = [
        (chunk + place * STEP_WIDTH, chunk, place, name)
        for chunk in range(CHUNKS)
        for place, name in enumerate(names(chunk))
    ]
    return [(chunk, name) for _, chunk, _, name in sorted(timed)]


def gather_kernel(
    grad_ref, place_ref, down_ref, up_ref, held, rows, down, own_sem, down_sem, send, recv, peer_send, peer_recv
):
    z, x, y, c = place_of()
    width = held.shape[-1]
    here = (z * 2 + x) * 2 + y
    started = []

    def start(copy, when=None):
        if when is None:
            copy.start()
        else:
            pl.when(when)(copy.start)
        started.append((copy, when))

    def own_copy(chunk):
        return pltpu.make_async_copy(
            grad_ref.at[:, pl.ds(chunk * width, width)], held.at[chunk, c, here], own_sem.at[chunk]
        )

    def down_copy(chunk):
        return pltpu.make_async_copy(
            down_ref.at[:, pl.ds(chunk * width, width)], down.at[chunk % 2], down_sem.at[chunk]
        )

    def multiply(chunk, core):
        @pl.loop(0, BLOCKS)
        def _(b):
            rows[b] = jnp.dot(
                place_ref[core, b], held[chunk, core, b], preferred_element_type=jnp.float32
            ).astype(jnp.bfloat16)

        group = 4

        @pl.loop(0, BLOCKS // group)
        def _(i):
            picked = rows[pl.ds(i * group, group)]
            term = lax.dot_general(
                picked.reshape(-1, width),
                down[chunk % 2],
                (((1,), (1,)), ((), ())),
                preferred_element_type=jnp.float32,
            ).reshape(group, -1, down.shape[1])
            if chunk == 0:
                up_ref[core, pl.ds(i * group, group)] = term
            else:
                up_ref[core, pl.ds(i * group, group)] += term

    def step(chunk, name):
        kind, k = name
        z_first, swap = CHUNK_ORDERS[chunk]
        near = Copies(swap)
        p, q = near.p, near.q

        def spread(block, index, dz=None, dp=0, dq=0, when=None):
            ref = held.at[chunk, c, block]
            start(
                near.remote(
                    ref,
                    ref,
                    send.at[chunk, index],
                    recv.at[chunk, block],
                    z if dz is None else z + dz,
                    1 - p if dp else p,
                    1 - q if dq else q,
                ),
                when,
            )

        def arrived(block):
            ref = held.at[chunk, c, block]
            near.remote(ref, ref, send.at[chunk, 0], recv.at[chunk, block], z, 1 - p, q).wait_recv()

        def both_ways(block, index):
            spread(block, index, dz=1, when=z < LEVELS - 1)
            spread(block, index + 1, dz=-1, when=z > 0)

        def onward(block, level, index):
            up = level < z
            spread(
                block,
                index,
                dz=jnp.where(up, 1, -1),
                when=jnp.where(up, z < LEVELS - 1, z > 0),
            )

        level = nearest(z, k)
        if kind == "own":
            own_copy(chunk).wait()
            block = near.block(z, p, q)
            if z_first:
                both_ways(block, 0)
                spread(block, 5, dp=1)
                spread(block, 9, dq=1)
            else:
                spread(block, 0, dp=1)
                both_ways(block, 1)
                spread(block, 11, dq=1)
        elif kind == "Z":
            block = near.block(level, p, q)
            arrived(block)
            if z_first:
                onward(block, level, 1 + k)
                spread(block, 5 + k, dp=1)
                spread(block, 9 + k, dq=1)
            else:
                onward(block, level, 2 + k)
                spread(block, 11 + k, dq=1)
        elif kind == "P":
            block = near.block(level, 1 - p, q)
            arrived(block)
            if z_first:
                spread(block, 13 + k, dq=1)
            else:
                both_ways(block, 6)
                spread(block, 15, dq=1)
        elif kind == "Y":
            block = near.block(level, 1 - p, q)
            arrived(block)
            onward(block, level, 7 + k)
            spread(block, 15 + k, dq=1)
        elif kind == "Q":
            for other in range(LEVELS):
                for side in range(2):
                    arrived(near.block(other, side, 1 - q))
            ref = held.at[chunk, c]
            start(sibling_copy(ref, ref, peer_send.at[chunk], peer_recv.at[chunk]))
        elif kind == "near":
            down_copy(chunk).wait()
            multiply(chunk, c)
        elif kind == "far":
            ref = held.at[chunk, 1 - c]
            sibling_copy(ref, ref, peer_send.at[chunk], peer_recv.at[chunk]).wait_recv()
            multiply(chunk, 1 - c)
            if chunk + 2 < CHUNKS:
                down_copy(chunk + 2).start()

    for chunk in range(CHUNKS):
        own_copy(chunk).start()
    down_copy(0).start()
    down_copy(1).start()
    for chunk, name in pipelined(gather_names):
        step(chunk, name)
    for copy, when in started:
        if when is None:
            copy.wait_send()
        else:
            pl.when(when)(copy.wait_send)


def gather_call(grad, place, down_weight):
    rows, model_width = grad.shape
    hidden = down_weight.shape[0]
    capacity = place.shape[2]
    width = model_width // CHUNKS
    dma = pltpu.SemaphoreType.DMA
    return pl.pallas_call(
        gather_kernel,
        out_shape=jax.ShapeDtypeStruct((2, BLOCKS, capacity, hidden), jnp.float32),
        in_specs=[
            pl.BlockSpec(memory_space=pl.ANY),
            pl.BlockSpec(memory_space=pltpu.VMEM),
            pl.BlockSpec(memory_space=pl.ANY),
        ],
        out_specs=pl.BlockSpec(memory_space=pltpu.VMEM),
        scratch_shapes=[
            pltpu.VMEM((CHUNKS, 2, BLOCKS, rows, width), jnp.bfloat16),
            pltpu.VMEM((BLOCKS, capacity, width), jnp.bfloat16),
            pltpu.VMEM((2, hidden, width), jnp.bfloat16),
            dma((CHUNKS,)),
            dma((CHUNKS,)),
            dma((CHUNKS, 19)),
            dma((CHUNKS, BLOCKS)),
            dma((CHUNKS,)),
            dma((CHUNKS,)),
        ],
        compiler_params=pltpu.CompilerParams(
            has_side_effects=True, vmem_limit_bytes=60 * 2**20
        ),
        name="gather_upstream",
    )(grad, place, down_weight)


def return_names(chunk):
    if CHUNK_ORDERS[chunk][0]:
        middle = [("P", k) for k in (3, 2, 1, 0)] + [("Z", k) for k in (3, 2, 1)]
    else:
        middle = [("Y", k) for k in (3, 2, 1)] + [("Z", k) for k in (3, 2, 1)] + [("P", 0)]
    return [("away", 0), ("near", 0)] + middle + [("own", 0)]


def return_kernel(
    first_ref,
    second_ref,
    join_ref,
    gate_ref,
    up_ref,
    out_ref,
    held,
    landed,
    leaving,
    weights,
    weight_sem,
    send,
    recv,
    peer_send,
    peer_recv,
):
    z, x, y, c = place_of()
    capacity = first_ref.shape[2]
    width = held.shape[-1]
    hidden = first_ref.shape[3]
    started = []

    def start(copy, when=None):
        if when is None:
            copy.start()
        else:
            pl.when(when)(copy.start)
        started.append((copy, when))

    def weight_copies(chunk):
        return [
            pltpu.make_async_copy(
                ref.at[pl.ds(chunk * width, width)],
                weights.at[chunk % 2, i],
                weight_sem.at[chunk, i],
            )
            for i, ref in enumerate((gate_ref, up_ref))
        ]

    def back_rows(chunk, core, store):
        group = 4

        @pl.loop(0, BLOCKS // group)
        def _(i):
            total = None
            for j, ref in enumerate((first_ref, second_ref)):
                term = lax.dot_general(
                    ref[core, pl.ds(i * group, group)].reshape(-1, hidden),
                    weights[chunk % 2, j],
                    (((1,), (1,)), ((), ())),
                    preferred_element_type=jnp.float32,
                )
                total = term if total is None else total + term
            store(i * group, group, total.astype(jnp.bfloat16).reshape(group, capacity, width))

    def leave(chunk):
        return sibling_copy(
            leaving.at[chunk % 2],
            held.at[chunk, :, pl.ds(capacity, capacity)],
            peer_send.at[chunk],
            peer_recv.at[chunk],
        )

    def step(chunk, name):
        kind, k = name
        z_first, swap = CHUNK_ORDERS[chunk]
        near = Copies(swap)
        p, q = near.p, near.q

        def give(block, slot, index, dz=None, dp=0, dq=0, when=None):
            start(
                near.remote(
                    held.at[chunk, block],
                    landed.at[chunk, slot],
                    send.at[chunk, index],
                    recv.at[chunk, slot],
                    z if dz is None else z + dz,
                    1 - p if dp else p,
                    1 - q if dq else q,
                ),
                when,
            )

        def take(block, slot):
            ref = landed.at[chunk, slot]
            near.remote(ref, ref, send.at[chunk, 0], recv.at[chunk, slot], z, 1 - p, q).wait_recv()
            held[chunk, block] = (
                held[chunk, block].astype(jnp.float32) + landed[chunk, slot].astype(jnp.float32)
            ).astype(jnp.bfloat16)

        def take_outer(block, level, base):
            pl.when(jnp.where(level > z, z > 0, z < LEVELS - 1))(lambda: take(block, base + level))

        def give_inner(block, level, base, index):
            up = level > z
            last = level == z - 1
            give(
                block,
                base + jnp.where(last, LEVELS, level),
                index,
                dz=jnp.where(up, 1, -1),
            )

        def take_ends(block, base):
            pl.when(z > 0)(lambda: take(block, base + z))
            pl.when(z < LEVELS - 1)(lambda: take(block, base + LEVELS))

        level = nearest(z, k)
        if kind == "away":
            for copy in weight_copies(chunk):
                copy.wait()
            if chunk >= 2:
                leave(chunk - 2).wait_send()

            def store(at, count, value):
                leaving[chunk % 2, pl.ds(at, count)] = value

            back_rows(chunk, 1 - c, store)
            leave(chunk).start()
        elif kind == "near":

            def store(at, count, value):
                held[chunk, pl.ds(at, count), pl.ds(0, capacity)] = value

            back_rows(chunk, c, store)
            if chunk + 2 < CHUNKS:
                for copy in weight_copies(chunk + 2):
                    copy.start()
            leave(chunk).wait_recv()

            @pl.loop(0, BLOCKS)
            def _(b):
                held[chunk, b] = jnp.dot(
                    join_ref[b], held[chunk, b], preferred_element_type=jnp.float32
                ).astype(jnp.bfloat16)

            for side in (1, 0):
                for far in (3, 2, 1, 0):
                    other = nearest(z, far)
                    column = 1 - p if side else p
                    give(
                        near.block(other, column, 1 - q),
                        other * 2 + column,
                        far * 2 + side,
                        dq=1,
                    )
        elif kind == "P" and z_first:
            block = near.block(level, 1 - p, q)
            take(block, level * 2 + 1 - p)
            give(block, 8 + level, 8 + k, dp=1)
        elif kind == "P":
            block = near.block(z, 1 - p, q)
            take(block, z * 2 + 1 - p)
            take_ends(block, 13)
            give(block, 18, 14, dp=1)
        elif kind == "Z":
            block = near.block(level, p, q)
            take(block, level * 2 + p)
            if z_first:
                take(block, 8 + level)
                take_outer(block, level, 12)
                give_inner(block, level, 12, 11 + k)
            else:
                take_outer(block, level, 8)
                give_inner(block, level, 8, 7 + k)
        elif kind == "Y":
            block = near.block(level, 1 - p, q)
            take(block, level * 2 + 1 - p)
            take_outer(block, level, 13)
            give_inner(block, level, 13, 10 + k)
        elif kind == "own":
            block = near.block(z, p, q)
            take(block, z * 2 + p)
            if z_first:
                take(block, 8 + z)
                take_ends(block, 12)
            else:
                take_ends(block, 8)
                take(block, 18)
            out_ref[:, chunk * width : (chunk + 1) * width] = held[chunk, block]

    for chunk in range(2):
        for copy in weight_copies(chunk):
            copy.start()
    for chunk, name in pipelined(return_names):
        step(chunk, name)
    for chunk in range(CHUNKS - 2, CHUNKS):
        leave(chunk).wait_send()
    for copy, when in started:
        if when is None:
            copy.wait_send()
        else:
            pl.when(when)(copy.wait_send)


def return_call(first, second, joined, gate_weight, up_weight):
    model_width, hidden = gate_weight.shape
    capacity = first.shape[2]
    rows = joined.shape[1]
    width = model_width // CHUNKS
    dma = pltpu.SemaphoreType.DMA
    vmem, anywhere = pl.BlockSpec(memory_space=pltpu.VMEM), pl.BlockSpec(memory_space=pl.ANY)
    return pl.pallas_call(
        return_kernel,
        out_shape=jax.ShapeDtypeStruct((rows, model_width), jnp.bfloat16),
        in_specs=[vmem, vmem, vmem, anywhere, anywhere],
        out_specs=vmem,
        scratch_shapes=[
            pltpu.VMEM((CHUNKS, BLOCKS, rows, width), jnp.bfloat16),
            pltpu.VMEM((CHUNKS, 19, rows, width), jnp.bfloat16),
            pltpu.VMEM((2, BLOCKS, capacity, width), jnp.bfloat16),
            pltpu.VMEM((2, 2, width, hidden), jnp.bfloat16),
            dma((CHUNKS, 2)),
            dma((CHUNKS, 15)),
            dma((CHUNKS, 19)),
            dma((CHUNKS,)),
            dma((CHUNKS,)),
        ],
        compiler_params=pltpu.CompilerParams(
            has_side_effects=True, vmem_limit_bytes=60 * 2**20
        ),
        name="back_return",
    )(first, second, joined, gate_weight, up_weight)


def silu_terms(pre_gate, pre_up):
    first = pre_gate.astype(jnp.float32)
    second = pre_up.astype(jnp.float32)
    gate_sig = jax.nn.sigmoid(first)
    gate_act = first * gate_sig
    return second * gate_sig * (1.0 + first * (1.0 - gate_sig)), gate_act, gate_act * second


def gathered_shards(
    tokens,
    out_grad,
    router_weight,
    gate_weight,
    up_weight,
    down_weight,
    saved_gate,
    saved_up,
    expert_ids,
    aux_weight,
):
    both = ("seq", "exp")
    seq_size = lax.axis_size("seq")
    exp_size = lax.axis_size("exp")
    devices = seq_size * exp_size
    inputs = tokens[0]
    chosen_ids = expert_ids[0]
    tok_rows, top_count = chosen_ids.shape
    model_width = inputs.shape[1]
    experts = router_weight.shape[1]
    capacity = saved_gate.shape[1] // devices

    logits = jnp.dot(inputs, router_weight, preferred_element_type=jnp.float32)
    router_probs = jax.nn.softmax(logits, axis=-1)
    onehot = (chosen_ids[:, :, None] == jnp.arange(experts, dtype=jnp.int32)).astype(jnp.float32)
    picked = jnp.sum(onehot, axis=1)
    chosen_sum = jnp.sum(router_probs * picked, axis=1, keepdims=True)
    gate_dense = router_probs * picked / chosen_sum
    earlier = jnp.tril(jnp.ones((tok_rows, tok_rows), jnp.bfloat16), -1)
    rank = jnp.dot(earlier, picked.astype(jnp.bfloat16), preferred_element_type=jnp.float32)
    slot_pos = jnp.where(picked > 0, rank, -1.0)
    sent = jnp.stack([slot_pos.T, gate_dense.astype(jnp.bfloat16).astype(jnp.float32).T], axis=1)
    received = lax.all_to_all(sent, both, split_axis=0, concat_axis=0, tiled=True)

    counts = jnp.sum((received[:, 0] >= 0).astype(jnp.float32), axis=1)
    counts = jnp.tile(jnp.sum(counts.reshape(seq_size, exp_size), axis=0), seq_size)

    def by_core(value):
        return jnp.swapaxes(value.reshape((devices // 2, 2) + value.shape[1:]), 0, 1)

    here_core = lax.axis_index("exp") % 2
    pos = received[:, 0].astype(jnp.int32)
    slot_ids = jnp.arange(capacity, dtype=jnp.int32)[None, :, None]
    at_slot = pos[:, None, :] == slot_ids
    gate_rows = jnp.sum(jnp.where(at_slot, received[:, 1][:, None, :], 0.0), axis=2)[:, :, None]
    place = by_core(at_slot.astype(jnp.bfloat16))
    pos_by_core = by_core(received[:, 0])
    own_pos = lax.dynamic_index_in_dim(pos_by_core, here_core, 0, keepdims=False)
    sent_pos = lax.dynamic_index_in_dim(pos_by_core, 1 - here_core, 0, keepdims=False)
    other_pos = lax.ppermute(sent_pos, "exp", [(i, i ^ 1) for i in range(exp_size)])
    join_pos = jnp.concatenate(
        [
            jnp.broadcast_to(own_pos[:, :, None], (devices // 2, tok_rows, capacity)),
            jnp.broadcast_to(other_pos[:, :, None], (devices // 2, tok_rows, capacity)),
        ],
        axis=2,
    ).astype(jnp.int32)
    joined = (join_pos == jnp.arange(2 * capacity, dtype=jnp.int32) % capacity).astype(jnp.bfloat16)

    upstream = gather_call(out_grad[0], place, down_weight[0])

    hidden_width = saved_gate.shape[2]
    blocks = (devices, capacity, hidden_width)
    slope, gate_act, hidden = silu_terms(
        by_core(saved_gate[0].reshape(blocks)), by_core(saved_up[0].reshape(blocks))
    )
    slot_combine = jnp.sum(upstream * hidden, axis=-1).astype(jnp.bfloat16)
    scaled = by_core(gate_rows) * upstream
    grad_first = (scaled * slope).astype(jnp.bfloat16)
    grad_second = (scaled * gate_act).astype(jnp.bfloat16)

    slot_combine = jnp.swapaxes(slot_combine, 0, 1).reshape(devices, capacity)
    combine_tok = jnp.sum(
        jnp.where(at_slot, slot_combine.astype(jnp.float32)[:, :, None], 0.0), axis=1
    )
    reply = jnp.stack([combine_tok, jnp.broadcast_to(counts[:, None], combine_tok.shape)], axis=1)
    answered = lax.all_to_all(reply, both, split_axis=0, concat_axis=0, tiled=True)

    expert_sum = return_call(grad_first, grad_second, joined, gate_weight[0], up_weight[0])

    combine_dense = answered[:, 0].T
    seq_counts = answered[:, 1, 0]
    combine_grad = jnp.sum(onehot * combine_dense[:, None, :], axis=2)
    mixed = jnp.sum(gate_dense * combine_dense, axis=1, keepdims=True)
    prob_grad = picked * (combine_dense - mixed) / chosen_sum
    fraction = experts * seq_counts / (top_count * tok_rows * seq_size)
    prob_grad = prob_grad + aux_weight[0] * fraction[None, :]
    dlogits = router_probs * (prob_grad - jnp.sum(router_probs * prob_grad, axis=1, keepdims=True))
    logit_grad = dlogits.astype(jnp.bfloat16)

    router_terms = jnp.einsum("te,td->ed", logit_grad, inputs, preferred_element_type=jnp.float32)
    router_terms = router_terms.reshape(experts, devices, model_width // devices)
    router_terms = lax.all_to_all(
        router_terms.transpose(1, 0, 2), both, split_axis=0, concat_axis=0, tiled=True
    )
    router_grad = jnp.sum(router_terms, axis=0).T

    token_grad = expert_sum.astype(jnp.float32) + jnp.einsum(
        "te,de->td", logit_grad, router_weight, preferred_element_type=jnp.float32
    )
    return (token_grad.astype(jnp.bfloat16)[None], combine_grad[None], router_grad)


def program(*arrays):
    tok_rows = arrays[0].shape[1]
    seq_size, exp_size = lax.axis_size("seq"), lax.axis_size("exp")
    slots = arrays[6].shape[1]
    lined = exp_size == 4 and seq_size == 2 * LEVELS
    fits = arrays[0].shape[2] == 4096 and arrays[6].shape[2] == 768 and tok_rows == 128
    if lined and fits and seq_size * exp_size * tok_rows <= 2 * slots:
        return gathered_shards(*arrays)
    return shards(*arrays)


def solution(mesh):
    placed = (
        P("exp", "seq", None),
        P("exp", "seq", None),
        P(),
        P(("seq", "exp"), None, None),
        P(("seq", "exp"), None, None),
        P(("seq", "exp"), None, None),
        P(("seq", "exp"), None, None),
        P(("seq", "exp"), None, None),
        P("exp", "seq", None),
        P(),
    )
    return jax.shard_map(
        program,
        mesh=mesh,
        in_specs=placed,
        out_specs=(P("exp", "seq", None), P("exp", "seq", None), P(("seq", "exp"), None)),
        check_vma=False,
    )
```

```python
import jax
import jax.numpy as jnp
from jax import lax
from jax.experimental import pallas as pl
from jax.experimental.pallas import tpu as pltpu
from jax.sharding import PartitionSpec as P


def expert_backward(grad_rows, gate_rows, w_gate, w_up, w_down, pre_gate, pre_up):
    upstream = jnp.einsum("rd,fd->rf", grad_rows, w_down, preferred_element_type=jnp.float32)
    first = pre_gate.astype(jnp.float32)
    second = pre_up.astype(jnp.float32)
    gate_sig = jax.nn.sigmoid(first)
    gate_act = first * gate_sig
    hidden = gate_act * second
    slot_combine = jnp.sum(upstream * hidden, axis=-1).astype(jnp.bfloat16)
    scaled = gate_rows.astype(jnp.float32)[:, None] * upstream
    grad_first = (scaled * second * gate_sig * (1.0 + first * (1.0 - gate_sig))).astype(
        jnp.bfloat16
    )
    grad_second = (scaled * gate_act).astype(jnp.bfloat16)
    back_rows = jnp.einsum("rf,df->rd", grad_first, w_gate, preferred_element_type=jnp.float32)
    back_rows = back_rows + jnp.einsum(
        "rf,df->rd", grad_second, w_up, preferred_element_type=jnp.float32
    )
    return (back_rows.astype(jnp.bfloat16), slot_combine)


def shards(
    tokens,
    out_grad,
    router_weight,
    gate_weight,
    up_weight,
    down_weight,
    saved_gate,
    saved_up,
    expert_ids,
    aux_weight,
):
    seq_size = lax.axis_size("seq")
    exp_size = lax.axis_size("exp")
    devices = seq_size * exp_size
    inputs = tokens[0]
    upstream_grad = out_grad[0]
    chosen_ids = expert_ids[0]
    tok_rows, top_count = chosen_ids.shape
    model_width = inputs.shape[1]
    experts = router_weight.shape[1]
    capacity = saved_gate.shape[1] // devices
    logits = jnp.dot(inputs, router_weight, preferred_element_type=jnp.float32)
    router_probs = jax.nn.softmax(logits, axis=-1)
    chosen = jnp.take_along_axis(router_probs, chosen_ids, axis=1)
    chosen_sum = jnp.sum(chosen, axis=1, keepdims=True)
    gate_vals = chosen / chosen_sum
    onehot = (
        chosen_ids.reshape(-1)[:, None] == jnp.arange(experts, dtype=jnp.int32)[None, :]
    ).astype(jnp.int32)
    rank_before = jnp.cumsum(onehot, axis=0) - onehot
    slot_pos = jnp.sum(rank_before * onehot, axis=1)
    slot_index = chosen_ids.reshape(-1) * capacity + slot_pos
    token_order = jnp.arange(tok_rows * top_count, dtype=jnp.int32) // top_count
    slot_token = (
        jnp.full((experts * capacity,), tok_rows, jnp.int32).at[slot_index].set(token_order)
    )
    grad_padded = jnp.concatenate(
        [upstream_grad, jnp.zeros((1, model_width), jnp.bfloat16)], axis=0
    )
    grad_slots = grad_padded[slot_token]
    gate_slots = (
        jnp.zeros((experts * capacity,), jnp.bfloat16)
        .at[slot_index]
        .set(gate_vals.reshape(-1).astype(jnp.bfloat16))
    )
    chosen_count = jnp.sum(onehot.reshape(tok_rows, top_count, experts), axis=1).astype(jnp.float32)
    local_counts = jnp.sum(chosen_count, axis=0)
    seq_counts = lax.psum(local_counts, "seq")
    recv_grad, recv_gate = (
        lax.all_to_all(
            grad_slots.reshape(experts, 1, capacity, model_width),
            ("seq", "exp"),
            split_axis=0,
            concat_axis=1,
            tiled=True,
        ),
        lax.all_to_all(
            gate_slots.reshape(experts, 1, capacity),
            ("seq", "exp"),
            split_axis=0,
            concat_axis=1,
            tiled=True,
        ),
    )
    back_rows, slot_combine = expert_backward(
        recv_grad.reshape(-1, model_width),
        recv_gate.reshape(-1),
        gate_weight[0],
        up_weight[0],
        down_weight[0],
        saved_gate[0],
        saved_up[0],
    )
    returned, combine_back = (
        lax.all_to_all(
            back_rows.reshape(1, devices, capacity, model_width),
            ("seq", "exp"),
            split_axis=1,
            concat_axis=0,
            tiled=True,
        ),
        lax.all_to_all(
            slot_combine.reshape(1, devices, capacity),
            ("seq", "exp"),
            split_axis=1,
            concat_axis=0,
            tiled=True,
        ),
    )
    returned_rows = returned.reshape(experts * capacity, model_width)
    expert_sum = jnp.sum(
        returned_rows[slot_index].reshape(tok_rows, top_count, model_width).astype(jnp.float32),
        axis=1,
    )
    combine_grad = (
        combine_back.reshape(-1)[slot_index].reshape(tok_rows, top_count).astype(jnp.float32)
    )
    prob_sel = (
        combine_grad - jnp.sum(gate_vals * combine_grad, axis=1, keepdims=True)
    ) / chosen_sum
    prob_grad = jnp.einsum(
        "tk,tke->te", prob_sel, onehot.reshape(tok_rows, top_count, experts).astype(jnp.float32)
    )
    fraction = experts * seq_counts / (top_count * tok_rows * seq_size)
    prob_grad = prob_grad + aux_weight[0] * fraction[None, :]
    dlogits = router_probs * (prob_grad - jnp.sum(router_probs * prob_grad, axis=1, keepdims=True))
    logit_grad = dlogits.astype(jnp.bfloat16)
    token_grad = expert_sum + jnp.einsum(
        "te,de->td", logit_grad, router_weight, preferred_element_type=jnp.float32
    )
    router_grad = lax.psum_scatter(
        jnp.einsum("td,te->de", inputs, logit_grad, preferred_element_type=jnp.float32),
        ("seq", "exp"),
        scatter_dimension=0,
        tiled=True,
    )
    return (token_grad.astype(jnp.bfloat16)[None], combine_grad[None], router_grad)

MESH = pl.DeviceIdType.MESH
GATHER_TYPES = ((False, False), (False, True), (True, False), (False, True), (False, False), (True, True), (False, True), (False, False))
RETURN_TYPES = ((False, False), (False, True), (False, False), (False, True), (True, True), (True, False), (False, True), (False, False))
GATHER_ORDER = (
    60, 40, 80, 100, 20, 0, 101, 42, 41, 120, 22, 44, 21, 2, 102, 1, 23, 121, 140, 61, 43, 3, 24, 6,
    7, 5, 26, 25, 45, 81, 106, 62, 47, 4, 63, 103, 46, 65, 27, 85, 104, 8, 66, 142, 9, 86, 107, 83,
    82, 10, 28, 122, 64, 29, 84, 67, 125, 123, 105, 143, 48, 30, 87, 68, 141, 49, 69, 126, 50, 124,
    145, 88, 70, 89, 108, 146, 127, 109, 144, 90, 128, 147, 110, 129, 148, 149, 130, 150,
)
RETURN_ORDER = (
    0, 20, 1, 2, 3, 21, 22, 10, 27, 4, 26, 40, 6, 11, 23, 8, 28, 60, 12, 30, 41, 42, 13, 61, 67, 62,
    46, 33, 80, 50, 47, 100, 43, 45, 7, 5, 53, 24, 81, 31, 63, 120, 51, 82, 64, 34, 101, 140, 68,
    103, 48, 32, 85, 83, 54, 106, 107, 44, 70, 66, 121, 141, 105, 55, 146, 35, 108, 90, 124, 123,
    122, 14, 93, 73, 144, 128, 25, 84, 15, 130, 126, 102, 109, 86, 142, 74, 125, 127, 143, 36, 132,
    104, 72, 129, 65, 71, 9, 92, 29, 153, 110, 131, 52, 145, 113, 150, 56, 16, 151, 49, 111, 133,
    75, 112, 94, 88, 114, 76, 152, 87, 148, 91, 147, 57, 115, 136, 89, 149, 134, 69, 135, 37, 116,
    95, 156, 154, 96, 155, 117, 137, 17, 97, 77, 157,
)

CHUNKS = len(GATHER_TYPES)
LEVELS = 4
BLOCKS = 4 * LEVELS


def place_of():
    seq, exp = lax.axis_index("seq"), lax.axis_index("exp")
    return seq // 2, seq % 2, exp // 2, exp % 2


def nearest(z, k):
    table = ((0, 1, 2, 3), (1, 2, 0, 3), (2, 1, 3, 0), (3, 2, 1, 0))
    value = jnp.int32(table[3][k])
    for level in (2, 1, 0):
        value = jnp.where(z == level, jnp.int32(table[level][k]), value)
    return value


def planar(first, second, swap):
    return (second, first) if swap else (first, second)


class Copies:
    def __init__(self, swap):
        self.z, self.x, self.y, self.c = place_of()
        self.swap = swap
        self.p, self.q = planar(self.x, self.y, swap)

    def block(self, z, p, q):
        x, y = planar(p, q, self.swap)
        return (z * 2 + x) * 2 + y

    def device(self, z, p, q):
        x, y = planar(p, q, self.swap)
        return z * 2 + x, y * 2 + self.c

    def remote(self, src, dst, send, recv, z, p, q):
        return pltpu.make_async_remote_copy(
            src_ref=src,
            dst_ref=dst,
            send_sem=send,
            recv_sem=recv,
            device_id=self.device(z, p, q),
            device_id_type=MESH,
        )


def sibling_copy(src, dst, send, recv):
    z, x, y, c = place_of()
    return pltpu.make_async_remote_copy(
        src_ref=src,
        dst_ref=dst,
        send_sem=send,
        recv_sem=recv,
        device_id=(z * 2 + x, y * 2 + 1 - c),
        device_id_type=MESH,
    )


def gather_names(chunk):
    if GATHER_TYPES[chunk][0]:
        middle = [("Z", k) for k in (1, 2, 3)] + [("P", k) for k in range(4)]
    else:
        middle = [("P", 0)] + [("Z", k) for k in (1, 2, 3)] + [("Y", k) for k in (1, 2, 3)]
    return [("own", 0)] + middle + [("Q", 0), ("near", 0), ("far", 0)]


def listed(order, names):
    return [(code // 20, names(code // 20)[code % 20]) for code in order]


def gather_kernel(
    grad_ref, place_ref, down_ref, up_ref, held, rows, down, own_sem, down_sem, send, recv, peer_send, peer_recv
):
    z, x, y, c = place_of()
    width = held.shape[-1]
    here = (z * 2 + x) * 2 + y
    started = []

    def start(copy, when=None):
        if when is None:
            copy.start()
        else:
            pl.when(when)(copy.start)
        started.append((copy, when))

    def own_copy(chunk):
        return pltpu.make_async_copy(
            grad_ref.at[:, pl.ds(chunk * width, width)], held.at[chunk, c, here], own_sem.at[chunk]
        )

    def down_copy(chunk):
        return pltpu.make_async_copy(
            down_ref.at[:, pl.ds(chunk * width, width)], down.at[chunk % 2], down_sem.at[chunk]
        )

    def multiply(chunk, core):
        @pl.loop(0, BLOCKS, unroll=4)
        def _(b):
            rows[b] = jnp.dot(
                place_ref[core, b], held[chunk, core, b], preferred_element_type=jnp.float32
            ).astype(jnp.bfloat16)

        group = 4

        @pl.loop(0, BLOCKS // group)
        def _(i):
            picked = rows[pl.ds(i * group, group)]
            term = lax.dot_general(
                picked.reshape(-1, width),
                down[chunk % 2],
                (((1,), (1,)), ((), ())),
                preferred_element_type=jnp.float32,
            ).reshape(group, -1, down.shape[1])
            if chunk == 0:
                up_ref[core, pl.ds(i * group, group)] = term
            else:
                up_ref[core, pl.ds(i * group, group)] += term

    def step(chunk, name):
        kind, k = name
        z_first, swap = GATHER_TYPES[chunk]
        near = Copies(swap)
        p, q = near.p, near.q

        def spread(block, index, dz=None, dp=0, dq=0, when=None):
            ref = held.at[chunk, c, block]
            start(
                near.remote(
                    ref,
                    ref,
                    send.at[chunk, index],
                    recv.at[chunk, block],
                    z if dz is None else z + dz,
                    1 - p if dp else p,
                    1 - q if dq else q,
                ),
                when,
            )

        def arrived(block):
            ref = held.at[chunk, c, block]
            near.remote(ref, ref, send.at[chunk, 0], recv.at[chunk, block], z, 1 - p, q).wait_recv()

        def both_ways(block, index):
            spread(block, index, dz=1, when=z < LEVELS - 1)
            spread(block, index + 1, dz=-1, when=z > 0)

        def onward(block, level, index):
            up = level < z
            spread(
                block,
                index,
                dz=jnp.where(up, 1, -1),
                when=jnp.where(up, z < LEVELS - 1, z > 0),
            )

        level = nearest(z, k)
        if kind == "own":
            own_copy(chunk).wait()
            block = near.block(z, p, q)
            if z_first:
                both_ways(block, 0)
                spread(block, 5, dp=1)
                spread(block, 9, dq=1)
            else:
                spread(block, 0, dp=1)
                both_ways(block, 1)
                spread(block, 11, dq=1)
        elif kind == "Z":
            block = near.block(level, p, q)
            arrived(block)
            if z_first:
                onward(block, level, 1 + k)
                spread(block, 5 + k, dp=1)
                spread(block, 9 + k, dq=1)
            else:
                onward(block, level, 2 + k)
                spread(block, 11 + k, dq=1)
        elif kind == "P":
            block = near.block(level, 1 - p, q)
            arrived(block)
            if z_first:
                spread(block, 13 + k, dq=1)
            else:
                both_ways(block, 6)
                spread(block, 15, dq=1)
        elif kind == "Y":
            block = near.block(level, 1 - p, q)
            arrived(block)
            onward(block, level, 7 + k)
            spread(block, 15 + k, dq=1)
        elif kind == "Q":
            for other in range(LEVELS):
                for side in range(2):
                    arrived(near.block(other, side, 1 - q))
            ref = held.at[chunk, c]
            start(sibling_copy(ref, ref, peer_send.at[chunk], peer_recv.at[chunk]))
        elif kind == "near":
            down_copy(chunk).wait()
            multiply(chunk, c)
        elif kind == "far":
            ref = held.at[chunk, 1 - c]
            sibling_copy(ref, ref, peer_send.at[chunk], peer_recv.at[chunk]).wait_recv()
            multiply(chunk, 1 - c)
            if chunk + 2 < CHUNKS:
                down_copy(chunk + 2).start()

    for chunk in range(CHUNKS):
        own_copy(chunk).start()
    down_copy(0).start()
    down_copy(1).start()
    for chunk, name in listed(GATHER_ORDER, gather_names):
        step(chunk, name)
    for copy, when in started:
        if when is None:
            copy.wait_send()
        else:
            pl.when(when)(copy.wait_send)


def gather_call(grad, place, down_weight):
    rows, model_width = grad.shape
    hidden = down_weight.shape[0]
    capacity = place.shape[2]
    width = model_width // CHUNKS
    dma = pltpu.SemaphoreType.DMA
    return pl.pallas_call(
        gather_kernel,
        out_shape=jax.ShapeDtypeStruct((2, BLOCKS, capacity, hidden), jnp.float32),
        in_specs=[
            pl.BlockSpec(memory_space=pl.ANY),
            pl.BlockSpec(memory_space=pltpu.VMEM),
            pl.BlockSpec(memory_space=pl.ANY),
        ],
        out_specs=pl.BlockSpec(memory_space=pltpu.VMEM),
        scratch_shapes=[
            pltpu.VMEM((CHUNKS, 2, BLOCKS, rows, width), jnp.bfloat16),
            pltpu.VMEM((BLOCKS, capacity, width), jnp.bfloat16),
            pltpu.VMEM((2, hidden, width), jnp.bfloat16),
            dma((CHUNKS,)),
            dma((CHUNKS,)),
            dma((CHUNKS, 19)),
            dma((CHUNKS, BLOCKS)),
            dma((CHUNKS,)),
            dma((CHUNKS,)),
        ],
        compiler_params=pltpu.CompilerParams(
            has_side_effects=True, vmem_limit_bytes=60 * 2**20
        ),
        name="gather_upstream",
    )(grad, place, down_weight)


def return_names(chunk):
    if RETURN_TYPES[chunk][0]:
        middle = [("P", k) for k in (3, 2, 1, 0)] + [("Z", k) for k in (3, 2, 1)]
    else:
        middle = [("Y", k) for k in (3, 2, 1)] + [("Z", k) for k in (3, 2, 1)] + [("P", 0)]
    leaves = [("leaf", (side, k)) for side in (1, 0) for k in (3, 2, 1, 0)]
    return [("away", 0), ("near", 0)] + leaves + middle + [("own", 0)]


def return_kernel(
    first_ref,
    second_ref,
    join_ref,
    gate_ref,
    up_ref,
    out_ref,
    held,
    landed,
    leaving,
    weights,
    weight_sem,
    send,
    recv,
    peer_send,
    peer_recv,
):
    z, x, y, c = place_of()
    capacity = first_ref.shape[2]
    width = held.shape[-1]
    hidden = first_ref.shape[3]
    started = []

    def start(copy, when=None):
        if when is None:
            copy.start()
        else:
            pl.when(when)(copy.start)
        started.append((copy, when))

    def weight_copies(chunk):
        return [
            pltpu.make_async_copy(
                ref.at[pl.ds(chunk * width, width)],
                weights.at[chunk % 2, i],
                weight_sem.at[chunk, i],
            )
            for i, ref in enumerate((gate_ref, up_ref))
        ]

    def back_rows(chunk, core, store):
        group = 4

        @pl.loop(0, BLOCKS // group)
        def _(i):
            total = None
            for j, ref in enumerate((first_ref, second_ref)):
                term = lax.dot_general(
                    ref[core, pl.ds(i * group, group)].reshape(-1, hidden),
                    weights[chunk % 2, j],
                    (((1,), (1,)), ((), ())),
                    preferred_element_type=jnp.float32,
                )
                total = term if total is None else total + term
            store(i * group, group, total.astype(jnp.bfloat16).reshape(group, capacity, width))

    def leave(chunk):
        return sibling_copy(
            leaving.at[chunk % 2],
            held.at[chunk, :, pl.ds(capacity, capacity)],
            peer_send.at[chunk],
            peer_recv.at[chunk],
        )

    def step(chunk, name):
        kind, k = name
        z_first, swap = RETURN_TYPES[chunk]
        near = Copies(swap)
        p, q = near.p, near.q

        def give(block, slot, index, dz=None, dp=0, dq=0, when=None):
            start(
                near.remote(
                    held.at[chunk, block],
                    landed.at[chunk, slot],
                    send.at[chunk, index],
                    recv.at[chunk, slot],
                    z if dz is None else z + dz,
                    1 - p if dp else p,
                    1 - q if dq else q,
                ),
                when,
            )

        def take(block, slot):
            ref = landed.at[chunk, slot]
            near.remote(ref, ref, send.at[chunk, 0], recv.at[chunk, slot], z, 1 - p, q).wait_recv()
            held[chunk, block] = (
                held[chunk, block].astype(jnp.float32) + landed[chunk, slot].astype(jnp.float32)
            ).astype(jnp.bfloat16)

        def take_outer(block, level, base):
            pl.when(jnp.where(level > z, z > 0, z < LEVELS - 1))(lambda: take(block, base + level))

        def give_inner(block, level, base, index):
            up = level > z
            last = level == z - 1
            give(
                block,
                base + jnp.where(last, LEVELS, level),
                index,
                dz=jnp.where(up, 1, -1),
            )

        def take_ends(block, base):
            pl.when(z > 0)(lambda: take(block, base + z))
            pl.when(z < LEVELS - 1)(lambda: take(block, base + LEVELS))

        level = None if kind == "leaf" else nearest(z, k)
        if kind == "away":
            for copy in weight_copies(chunk):
                copy.wait()
            if chunk >= 2:
                leave(chunk - 2).wait_send()

            def store(at, count, value):
                leaving[chunk % 2, pl.ds(at, count)] = value

            back_rows(chunk, 1 - c, store)
            leave(chunk).start()
        elif kind == "near":

            def store(at, count, value):
                held[chunk, pl.ds(at, count), pl.ds(0, capacity)] = value

            back_rows(chunk, c, store)
            if chunk + 2 < CHUNKS:
                for copy in weight_copies(chunk + 2):
                    copy.start()
            leave(chunk).wait_recv()

            @pl.loop(0, BLOCKS, unroll=4)
            def _(b):
                held[chunk, b] = jnp.dot(
                    join_ref[b], held[chunk, b], preferred_element_type=jnp.float32
                ).astype(jnp.bfloat16)
        elif kind == "leaf":
            side, far = k
            level = nearest(z, far)
            column = 1 - p if side else p
            give(near.block(level, column, 1 - q), level * 2 + column, far * 2 + side, dq=1)
        elif kind == "P" and z_first:
            block = near.block(level, 1 - p, q)
            take(block, level * 2 + 1 - p)
            give(block, 8 + level, 8 + k, dp=1)
        elif kind == "P":
            block = near.block(z, 1 - p, q)
            take(block, z * 2 + 1 - p)
            take_ends(block, 13)
            give(block, 18, 14, dp=1)
        elif kind == "Z":
            block = near.block(level, p, q)
            take(block, level * 2 + p)
            if z_first:
                take(block, 8 + level)
                take_outer(block, level, 12)
                give_inner(block, level, 12, 11 + k)
            else:
                take_outer(block, level, 8)
                give_inner(block, level, 8, 7 + k)
        elif kind == "Y":
            block = near.block(level, 1 - p, q)
            take(block, level * 2 + 1 - p)
            take_outer(block, level, 13)
            give_inner(block, level, 13, 10 + k)
        elif kind == "own":
            block = near.block(z, p, q)
            take(block, z * 2 + p)
            if z_first:
                take(block, 8 + z)
                take_ends(block, 12)
            else:
                take_ends(block, 8)
                take(block, 18)
            out_ref[:, chunk * width : (chunk + 1) * width] = held[chunk, block]

    for chunk in range(2):
        for copy in weight_copies(chunk):
            copy.start()
    for chunk, name in listed(RETURN_ORDER, return_names):
        step(chunk, name)
    for chunk in range(CHUNKS - 2, CHUNKS):
        leave(chunk).wait_send()
    for copy, when in started:
        if when is None:
            copy.wait_send()
        else:
            pl.when(when)(copy.wait_send)


def return_call(first, second, joined, gate_weight, up_weight):
    model_width, hidden = gate_weight.shape
    capacity = first.shape[2]
    rows = joined.shape[1]
    width = model_width // CHUNKS
    dma = pltpu.SemaphoreType.DMA
    vmem, anywhere = pl.BlockSpec(memory_space=pltpu.VMEM), pl.BlockSpec(memory_space=pl.ANY)
    return pl.pallas_call(
        return_kernel,
        out_shape=jax.ShapeDtypeStruct((rows, model_width), jnp.bfloat16),
        in_specs=[vmem, vmem, vmem, anywhere, anywhere],
        out_specs=vmem,
        scratch_shapes=[
            pltpu.VMEM((CHUNKS, BLOCKS, rows, width), jnp.bfloat16),
            pltpu.VMEM((CHUNKS, 19, rows, width), jnp.bfloat16),
            pltpu.VMEM((2, BLOCKS, capacity, width), jnp.bfloat16),
            pltpu.VMEM((2, 2, width, hidden), jnp.bfloat16),
            dma((CHUNKS, 2)),
            dma((CHUNKS, 15)),
            dma((CHUNKS, 19)),
            dma((CHUNKS,)),
            dma((CHUNKS,)),
        ],
        compiler_params=pltpu.CompilerParams(
            has_side_effects=True, vmem_limit_bytes=60 * 2**20
        ),
        name="back_return",
    )(first, second, joined, gate_weight, up_weight)


def silu_terms(pre_gate, pre_up):
    first = pre_gate.astype(jnp.float32)
    second = pre_up.astype(jnp.float32)
    gate_sig = jax.nn.sigmoid(first)
    gate_act = first * gate_sig
    return second * gate_sig * (1.0 + first * (1.0 - gate_sig)), gate_act, gate_act * second


def gathered_shards(
    tokens,
    out_grad,
    router_weight,
    gate_weight,
    up_weight,
    down_weight,
    saved_gate,
    saved_up,
    expert_ids,
    aux_weight,
):
    both = ("seq", "exp")
    seq_size = lax.axis_size("seq")
    exp_size = lax.axis_size("exp")
    devices = seq_size * exp_size
    inputs = tokens[0]
    chosen_ids = expert_ids[0]
    tok_rows, top_count = chosen_ids.shape
    model_width = inputs.shape[1]
    experts = router_weight.shape[1]
    capacity = saved_gate.shape[1] // devices

    logits = jnp.dot(inputs, router_weight, preferred_element_type=jnp.float32)
    router_probs = jax.nn.softmax(logits, axis=-1)
    onehot = (chosen_ids[:, :, None] == jnp.arange(experts, dtype=jnp.int32)).astype(jnp.float32)
    picked = jnp.sum(onehot, axis=1)
    chosen_sum = jnp.sum(router_probs * picked, axis=1, keepdims=True)
    gate_dense = router_probs * picked / chosen_sum
    earlier = jnp.tril(jnp.ones((tok_rows, tok_rows), jnp.bfloat16), -1)
    rank = jnp.dot(earlier, picked.astype(jnp.bfloat16), preferred_element_type=jnp.float32)
    slot_pos = jnp.where(picked > 0, rank, -1.0)
    sent = jnp.stack([slot_pos.T, gate_dense.astype(jnp.bfloat16).astype(jnp.float32).T], axis=1)
    received = lax.all_to_all(sent, both, split_axis=0, concat_axis=0, tiled=True)

    counts = jnp.sum((received[:, 0] >= 0).astype(jnp.float32), axis=1)
    counts = jnp.tile(jnp.sum(counts.reshape(seq_size, exp_size), axis=0), seq_size)

    def by_core(value):
        return jnp.swapaxes(value.reshape((devices // 2, 2) + value.shape[1:]), 0, 1)

    here_core = lax.axis_index("exp") % 2
    pos = received[:, 0].astype(jnp.int32)
    slot_ids = jnp.arange(capacity, dtype=jnp.int32)[None, :, None]
    at_slot = pos[:, None, :] == slot_ids
    gate_rows = jnp.sum(jnp.where(at_slot, received[:, 1][:, None, :], 0.0), axis=2)[:, :, None]
    place = by_core(at_slot.astype(jnp.bfloat16))
    pos_by_core = by_core(received[:, 0])
    own_pos = lax.dynamic_index_in_dim(pos_by_core, here_core, 0, keepdims=False)
    sent_pos = lax.dynamic_index_in_dim(pos_by_core, 1 - here_core, 0, keepdims=False)
    other_pos = lax.ppermute(sent_pos, "exp", [(i, i ^ 1) for i in range(exp_size)])
    join_pos = jnp.concatenate(
        [
            jnp.broadcast_to(own_pos[:, :, None], (devices // 2, tok_rows, capacity)),
            jnp.broadcast_to(other_pos[:, :, None], (devices // 2, tok_rows, capacity)),
        ],
        axis=2,
    ).astype(jnp.int32)
    joined = (join_pos == jnp.arange(2 * capacity, dtype=jnp.int32) % capacity).astype(jnp.bfloat16)

    upstream = gather_call(out_grad[0], place, down_weight[0])

    hidden_width = saved_gate.shape[2]
    blocks = (devices, capacity, hidden_width)
    slope, gate_act, hidden = silu_terms(
        by_core(saved_gate[0].reshape(blocks)), by_core(saved_up[0].reshape(blocks))
    )
    slot_combine = jnp.sum(upstream * hidden, axis=-1).astype(jnp.bfloat16)
    scaled = by_core(gate_rows) * upstream
    grad_first = (scaled * slope).astype(jnp.bfloat16)
    grad_second = (scaled * gate_act).astype(jnp.bfloat16)

    slot_combine = jnp.swapaxes(slot_combine, 0, 1).reshape(devices, capacity)
    combine_tok = jnp.sum(
        jnp.where(at_slot, slot_combine.astype(jnp.float32)[:, :, None], 0.0), axis=1
    )
    reply = jnp.stack([combine_tok, jnp.broadcast_to(counts[:, None], combine_tok.shape)], axis=1)
    answered = lax.all_to_all(reply, both, split_axis=0, concat_axis=0, tiled=True)

    expert_sum = return_call(grad_first, grad_second, joined, gate_weight[0], up_weight[0])

    combine_dense = answered[:, 0].T
    seq_counts = answered[:, 1, 0]
    combine_grad = jnp.sum(onehot * combine_dense[:, None, :], axis=2)
    mixed = jnp.sum(gate_dense * combine_dense, axis=1, keepdims=True)
    prob_grad = picked * (combine_dense - mixed) / chosen_sum
    fraction = experts * seq_counts / (top_count * tok_rows * seq_size)
    prob_grad = prob_grad + aux_weight[0] * fraction[None, :]
    dlogits = router_probs * (prob_grad - jnp.sum(router_probs * prob_grad, axis=1, keepdims=True))
    logit_grad = dlogits.astype(jnp.bfloat16)

    router_terms = jnp.einsum("te,td->ed", logit_grad, inputs, preferred_element_type=jnp.float32)
    router_terms = router_terms.reshape(experts, devices, model_width // devices)
    router_terms = lax.all_to_all(
        router_terms.transpose(1, 0, 2), both, split_axis=0, concat_axis=0, tiled=True
    )
    router_grad = jnp.sum(router_terms, axis=0).T

    token_grad = expert_sum.astype(jnp.float32) + jnp.einsum(
        "te,de->td", logit_grad, router_weight, preferred_element_type=jnp.float32
    )
    return (token_grad.astype(jnp.bfloat16)[None], combine_grad[None], router_grad)


def program(*arrays):
    tok_rows = arrays[0].shape[1]
    seq_size, exp_size = lax.axis_size("seq"), lax.axis_size("exp")
    slots = arrays[6].shape[1]
    lined = exp_size == 4 and seq_size == 2 * LEVELS
    fits = arrays[0].shape[2] == 4096 and arrays[6].shape[2] == 768 and tok_rows == 128
    if lined and fits and seq_size * exp_size * tok_rows <= 2 * slots:
        return gathered_shards(*arrays)
    return shards(*arrays)


def solution(mesh):
    placed = (
        P("exp", "seq", None),
        P("exp", "seq", None),
        P(),
        P(("seq", "exp"), None, None),
        P(("seq", "exp"), None, None),
        P(("seq", "exp"), None, None),
        P(("seq", "exp"), None, None),
        P(("seq", "exp"), None, None),
        P("exp", "seq", None),
        P(),
    )
    return jax.shard_map(
        program,
        mesh=mesh,
        in_specs=placed,
        out_specs=(P("exp", "seq", None), P("exp", "seq", None), P(("seq", "exp"), None)),
        check_vma=False,
    )
```

```python
import jax
import jax.numpy as jnp
from jax import lax
from jax.experimental import pallas as pl
from jax.experimental.pallas import tpu as pltpu
from jax.sharding import PartitionSpec as P


def expert_backward(grad_rows, gate_rows, w_gate, w_up, w_down, pre_gate, pre_up):
    upstream = jnp.einsum("rd,fd->rf", grad_rows, w_down, preferred_element_type=jnp.float32)
    first = pre_gate.astype(jnp.float32)
    second = pre_up.astype(jnp.float32)
    gate_sig = jax.nn.sigmoid(first)
    gate_act = first * gate_sig
    hidden = gate_act * second
    slot_combine = jnp.sum(upstream * hidden, axis=-1).astype(jnp.bfloat16)
    scaled = gate_rows.astype(jnp.float32)[:, None] * upstream
    grad_first = (scaled * second * gate_sig * (1.0 + first * (1.0 - gate_sig))).astype(
        jnp.bfloat16
    )
    grad_second = (scaled * gate_act).astype(jnp.bfloat16)
    back_rows = jnp.einsum("rf,df->rd", grad_first, w_gate, preferred_element_type=jnp.float32)
    back_rows = back_rows + jnp.einsum(
        "rf,df->rd", grad_second, w_up, preferred_element_type=jnp.float32
    )
    return (back_rows.astype(jnp.bfloat16), slot_combine)


def shards(
    tokens,
    out_grad,
    router_weight,
    gate_weight,
    up_weight,
    down_weight,
    saved_gate,
    saved_up,
    expert_ids,
    aux_weight,
):
    seq_size = lax.axis_size("seq")
    exp_size = lax.axis_size("exp")
    devices = seq_size * exp_size
    inputs = tokens[0]
    upstream_grad = out_grad[0]
    chosen_ids = expert_ids[0]
    tok_rows, top_count = chosen_ids.shape
    model_width = inputs.shape[1]
    experts = router_weight.shape[1]
    capacity = saved_gate.shape[1] // devices
    logits = jnp.dot(inputs, router_weight, preferred_element_type=jnp.float32)
    router_probs = jax.nn.softmax(logits, axis=-1)
    chosen = jnp.take_along_axis(router_probs, chosen_ids, axis=1)
    chosen_sum = jnp.sum(chosen, axis=1, keepdims=True)
    gate_vals = chosen / chosen_sum
    onehot = (
        chosen_ids.reshape(-1)[:, None] == jnp.arange(experts, dtype=jnp.int32)[None, :]
    ).astype(jnp.int32)
    rank_before = jnp.cumsum(onehot, axis=0) - onehot
    slot_pos = jnp.sum(rank_before * onehot, axis=1)
    slot_index = chosen_ids.reshape(-1) * capacity + slot_pos
    token_order = jnp.arange(tok_rows * top_count, dtype=jnp.int32) // top_count
    slot_token = (
        jnp.full((experts * capacity,), tok_rows, jnp.int32).at[slot_index].set(token_order)
    )
    grad_padded = jnp.concatenate(
        [upstream_grad, jnp.zeros((1, model_width), jnp.bfloat16)], axis=0
    )
    grad_slots = grad_padded[slot_token]
    gate_slots = (
        jnp.zeros((experts * capacity,), jnp.bfloat16)
        .at[slot_index]
        .set(gate_vals.reshape(-1).astype(jnp.bfloat16))
    )
    chosen_count = jnp.sum(onehot.reshape(tok_rows, top_count, experts), axis=1).astype(jnp.float32)
    local_counts = jnp.sum(chosen_count, axis=0)
    seq_counts = lax.psum(local_counts, "seq")
    recv_grad, recv_gate = (
        lax.all_to_all(
            grad_slots.reshape(experts, 1, capacity, model_width),
            ("seq", "exp"),
            split_axis=0,
            concat_axis=1,
            tiled=True,
        ),
        lax.all_to_all(
            gate_slots.reshape(experts, 1, capacity),
            ("seq", "exp"),
            split_axis=0,
            concat_axis=1,
            tiled=True,
        ),
    )
    back_rows, slot_combine = expert_backward(
        recv_grad.reshape(-1, model_width),
        recv_gate.reshape(-1),
        gate_weight[0],
        up_weight[0],
        down_weight[0],
        saved_gate[0],
        saved_up[0],
    )
    returned, combine_back = (
        lax.all_to_all(
            back_rows.reshape(1, devices, capacity, model_width),
            ("seq", "exp"),
            split_axis=1,
            concat_axis=0,
            tiled=True,
        ),
        lax.all_to_all(
            slot_combine.reshape(1, devices, capacity),
            ("seq", "exp"),
            split_axis=1,
            concat_axis=0,
            tiled=True,
        ),
    )
    returned_rows = returned.reshape(experts * capacity, model_width)
    expert_sum = jnp.sum(
        returned_rows[slot_index].reshape(tok_rows, top_count, model_width).astype(jnp.float32),
        axis=1,
    )
    combine_grad = (
        combine_back.reshape(-1)[slot_index].reshape(tok_rows, top_count).astype(jnp.float32)
    )
    prob_sel = (
        combine_grad - jnp.sum(gate_vals * combine_grad, axis=1, keepdims=True)
    ) / chosen_sum
    prob_grad = jnp.einsum(
        "tk,tke->te", prob_sel, onehot.reshape(tok_rows, top_count, experts).astype(jnp.float32)
    )
    fraction = experts * seq_counts / (top_count * tok_rows * seq_size)
    prob_grad = prob_grad + aux_weight[0] * fraction[None, :]
    dlogits = router_probs * (prob_grad - jnp.sum(router_probs * prob_grad, axis=1, keepdims=True))
    logit_grad = dlogits.astype(jnp.bfloat16)
    token_grad = expert_sum + jnp.einsum(
        "te,de->td", logit_grad, router_weight, preferred_element_type=jnp.float32
    )
    router_grad = lax.psum_scatter(
        jnp.einsum("td,te->de", inputs, logit_grad, preferred_element_type=jnp.float32),
        ("seq", "exp"),
        scatter_dimension=0,
        tiled=True,
    )
    return (token_grad.astype(jnp.bfloat16)[None], combine_grad[None], router_grad)

MESH = pl.DeviceIdType.MESH
GATHER_TYPES = ((False, False), (False, True), (True, False), (False, True), (False, False), (True, True), (False, True), (False, False))
RETURN_TYPES = ((False, False), (False, True), (False, False), (False, True), (True, True), (True, False), (False, True), (False, False))
GATHER_ORDER = (
    60, 40, 80, 100, 20, 0, 101, 42, 41, 120, 22, 44, 21, 2, 102, 1, 23, 121, 140, 61, 43, 3, 24, 6,
    7, 5, 26, 25, 45, 81, 106, 62, 47, 4, 63, 103, 46, 65, 27, 85, 104, 8, 66, 142, 9, 86, 107, 83,
    82, 10, 28, 122, 64, 29, 84, 67, 125, 123, 105, 143, 48, 30, 87, 68, 141, 49, 69, 126, 50, 124,
    145, 88, 70, 89, 108, 146, 127, 109, 144, 90, 128, 147, 110, 129, 148, 149, 130, 150,
)
RETURN_ORDER = (
    0, 20, 1, 2, 3, 21, 22, 10, 27, 4, 26, 40, 6, 11, 23, 8, 28, 60, 12, 30, 41, 42, 13, 61, 67, 62,
    46, 33, 80, 50, 47, 100, 43, 45, 7, 5, 53, 24, 81, 31, 63, 120, 51, 82, 64, 34, 101, 140, 68,
    103, 48, 32, 85, 83, 54, 106, 107, 44, 70, 66, 121, 141, 105, 55, 146, 35, 108, 90, 124, 123,
    122, 14, 93, 73, 144, 128, 25, 84, 15, 130, 126, 102, 109, 86, 142, 74, 125, 127, 143, 36, 132,
    104, 72, 129, 65, 71, 9, 92, 29, 153, 110, 131, 52, 145, 113, 150, 56, 16, 151, 49, 111, 133,
    75, 112, 94, 88, 114, 76, 152, 87, 148, 91, 147, 57, 115, 136, 89, 149, 134, 69, 135, 37, 116,
    95, 156, 154, 96, 155, 117, 137, 17, 97, 77, 157,
)

CHUNKS = len(GATHER_TYPES)
LEVELS = 4
AHEAD = 3
PARTS = 4
BLOCKS = 4 * LEVELS


def place_of():
    seq, exp = lax.axis_index("seq"), lax.axis_index("exp")
    return seq // 2, seq % 2, exp // 2, exp % 2


def nearest(z, k):
    table = ((0, 1, 2, 3), (1, 2, 0, 3), (2, 1, 3, 0), (3, 2, 1, 0))
    value = jnp.int32(table[3][k])
    for level in (2, 1, 0):
        value = jnp.where(z == level, jnp.int32(table[level][k]), value)
    return value


def planar(first, second, swap):
    return (second, first) if swap else (first, second)


class Copies:
    def __init__(self, swap):
        self.z, self.x, self.y, self.c = place_of()
        self.swap = swap
        self.p, self.q = planar(self.x, self.y, swap)

    def block(self, z, p, q):
        x, y = planar(p, q, self.swap)
        return (z * 2 + x) * 2 + y

    def device(self, z, p, q):
        x, y = planar(p, q, self.swap)
        return z * 2 + x, y * 2 + self.c

    def remote(self, src, dst, send, recv, z, p, q):
        return pltpu.make_async_remote_copy(
            src_ref=src,
            dst_ref=dst,
            send_sem=send,
            recv_sem=recv,
            device_id=self.device(z, p, q),
            device_id_type=MESH,
        )


def sibling_copy(src, dst, send, recv):
    z, x, y, c = place_of()
    return pltpu.make_async_remote_copy(
        src_ref=src,
        dst_ref=dst,
        send_sem=send,
        recv_sem=recv,
        device_id=(z * 2 + x, y * 2 + 1 - c),
        device_id_type=MESH,
    )


def gather_names(chunk):
    if GATHER_TYPES[chunk][0]:
        middle = [("Z", k) for k in (1, 2, 3)] + [("P", k) for k in range(4)]
    else:
        middle = [("P", 0)] + [("Z", k) for k in (1, 2, 3)] + [("Y", k) for k in (1, 2, 3)]
    return [("own", 0)] + middle + [("Q", 0), ("near", 0), ("far", 0)]


def listed(order, names):
    return [(code // 20, names(code // 20)[code % 20]) for code in order]


def route(token_ref, router_ref, id_ref, probs_ref, gate_ref, letter):
    experts, rows = probs_ref.shape
    logits = lax.dot_general(
        router_ref[...], token_ref[...], (((1,), (1,)), ((), ())), preferred_element_type=jnp.float32
    )
    shifted = jnp.exp(logits - jnp.max(logits, axis=0, keepdims=True))
    probs = shifted / jnp.sum(shifted, axis=0, keepdims=True)
    expert = lax.broadcasted_iota(jnp.int32, (experts, rows), 0)
    picked = jnp.zeros((experts, rows), jnp.float32)
    for k in range(id_ref.shape[0]):
        picked = picked + (id_ref[k : k + 1, :] == expert).astype(jnp.float32)
    chosen = probs * picked
    gates = chosen / jnp.sum(chosen, axis=0, keepdims=True)
    earlier = lax.broadcasted_iota(jnp.int32, (rows, rows), 0)
    earlier = (earlier < lax.broadcasted_iota(jnp.int32, (rows, rows), 1)).astype(jnp.float32)
    rank = jnp.dot(
        picked.astype(jnp.bfloat16),
        earlier.astype(jnp.bfloat16),
        preferred_element_type=jnp.float32,
    )
    slot_pos = jnp.where(picked > 0, rank, -1.0)
    sent_gates = gates.astype(jnp.bfloat16).astype(jnp.float32)
    probs_ref[...] = probs
    gate_ref[...] = gates
    for e in range(experts):
        letter[e, 0:1, :] = slot_pos[e : e + 1, :]
        letter[e, 1:2, :] = sent_gates[e : e + 1, :]
        letter[e, 2:3, :] = slot_pos[e ^ 1 : (e ^ 1) + 1, :]


class Mail:
    def __init__(self, outbox, inbox, send, recv):
        z, x, y, c = place_of()
        self.me = (z * 2 + x) * 4 + y * 2 + c
        self.outbox, self.inbox, self.send, self.recv = outbox, inbox, send, recv
        self.devices = outbox.shape[0]

    def copies(self):
        for step in range(1, self.devices):
            to = (self.me + step) % self.devices
            yield pltpu.make_async_remote_copy(
                src_ref=self.outbox.at[to],
                dst_ref=self.inbox.at[self.me],
                send_sem=self.send.at[step],
                recv_sem=self.recv.at[step],
                device_id=(to // 4, to % 4),
                device_id_type=MESH,
            )

    def post(self):
        self.inbox[self.me] = self.outbox[self.me]
        for copy in self.copies():
            copy.start()

    def collect(self):
        for step in range(1, self.devices):
            ref = self.inbox.at[(self.me - step + self.devices) % self.devices]
            pltpu.make_async_remote_copy(
                src_ref=ref,
                dst_ref=ref,
                send_sem=self.send.at[step],
                recv_sem=self.recv.at[step],
                device_id=(self.me // 4, self.me % 4),
                device_id_type=MESH,
            ).wait_recv()

    def close(self):
        for copy in self.copies():
            copy.wait_send()


def gather_kernel(
    grad_ref,
    down_ref,
    token_ref,
    router_ref,
    id_ref,
    pre_gate_ref,
    pre_up_ref,
    first_ref,
    second_ref,
    met_ref,
    reply,
    probs_ref,
    gate_ref,
    held,
    up_ref,
    rows,
    down,
    saved,
    grads,
    letter,
    inbox,
    own_sem,
    down_sem,
    saved_sem,
    grads_sem,
    send,
    recv,
    peer_send,
    peer_recv,
    mail_send,
    mail_recv,
):
    z, x, y, c = place_of()
    width = held.shape[-1]
    capacity = rows.shape[1]
    tok_rows = held.shape[-2]
    here = (z * 2 + x) * 2 + y
    started = []
    mail = Mail(letter, inbox, mail_send, mail_recv)

    def spots(core, b):
        slot = lax.broadcasted_iota(jnp.int32, (capacity, tok_rows), 0).astype(jnp.float32)
        return inbox[b * 2 + core, 0:1, :] == slot

    def saved_copies():
        return [
            pltpu.make_async_copy(ref, saved.at[i], saved_sem.at[i])
            for i, ref in enumerate((pre_gate_ref, pre_up_ref))
        ]

    def grad_copies(core, turn):
        return [
            pltpu.make_async_copy(grads.at[i, core], ref.at[core], grads_sem.at[turn, i])
            for i, ref in enumerate((first_ref, second_ref))
        ]

    def count():
        sources = inbox.shape[0]
        taken = (inbox[:, 0, :] >= 0).astype(jnp.bfloat16)
        one = lax.broadcasted_iota(jnp.int32, (sources, sources), 0) % 4
        two = lax.broadcasted_iota(jnp.int32, (sources, sources), 1) % 4
        alike = (one == two).astype(jnp.float32).astype(jnp.bfloat16)
        total = jnp.dot(alike, taken, preferred_element_type=jnp.float32)
        total = jnp.broadcast_to(jnp.sum(total, axis=1, keepdims=True), total.shape)
        for s in range(sources):
            reply[s, 1:2, :] = total[s : s + 1, :]

    def prepare(part):
        @pl.loop(part * BLOCKS // PARTS, (part + 1) * BLOCKS // PARTS)
        def _(b):
            for core in range(2):
                first = saved[0, b * 2 + core].astype(jnp.float32)
                second = saved[1, b * 2 + core].astype(jnp.float32)
                sig = jax.nn.sigmoid(first)
                grads[0, core, b] = (second * sig * (1.0 + first * (1.0 - sig))).astype(jnp.bfloat16)
                grads[1, core, b] = (first * sig).astype(jnp.bfloat16)

    def finish(core):
        @pl.loop(0, BLOCKS)
        def _(b):
            source = b * 2 + core
            upstream = up_ref[core, b]
            act = grads[1, core, b].astype(jnp.float32)
            at = spots(core, b)
            gate = jnp.sum(jnp.where(at, inbox[source, 1:2, :], 0.0), axis=1, keepdims=True)
            hidden = act * saved[1, source].astype(jnp.float32)
            combine = jnp.sum(upstream * hidden, axis=1, keepdims=True)
            combine = combine.astype(jnp.bfloat16).astype(jnp.float32)
            reply[source, 0:1, :] = jnp.sum(jnp.where(at, combine, 0.0), axis=0, keepdims=True)
            scaled = gate * upstream
            grads[0, core, b] = (scaled * grads[0, core, b].astype(jnp.float32)).astype(jnp.bfloat16)
            grads[1, core, b] = (scaled * act).astype(jnp.bfloat16)

    def start(copy, when=None):
        if when is None:
            copy.start()
        else:
            pl.when(when)(copy.start)
        started.append((copy, when))

    def own_copy(chunk):
        return pltpu.make_async_copy(
            grad_ref.at[:, pl.ds(chunk * width, width)], held.at[chunk, c, here], own_sem.at[chunk]
        )

    def down_copy(chunk):
        return pltpu.make_async_copy(
            down_ref.at[:, pl.ds(chunk * width, width)], down.at[chunk % 2], down_sem.at[chunk]
        )

    def multiply(chunk, core):
        @pl.loop(0, BLOCKS, unroll=4)
        def _(b):
            rows[b] = jnp.dot(
                spots(core, b).astype(jnp.float32).astype(jnp.bfloat16),
                held[chunk, core, b],
                preferred_element_type=jnp.float32,
            ).astype(jnp.bfloat16)

        group = 4

        @pl.loop(0, BLOCKS // group)
        def _(i):
            picked = rows[pl.ds(i * group, group)]
            term = lax.dot_general(
                picked.reshape(-1, width),
                down[chunk % 2],
                (((1,), (1,)), ((), ())),
                preferred_element_type=jnp.float32,
            ).reshape(group, -1, down.shape[1])
            if chunk == 0:
                up_ref[core, pl.ds(i * group, group)] = term
            else:
                up_ref[core, pl.ds(i * group, group)] += term

    def step(chunk, name):
        kind, k = name
        z_first, swap = GATHER_TYPES[chunk]
        near = Copies(swap)
        p, q = near.p, near.q

        def spread(block, index, dz=None, dp=0, dq=0, when=None):
            ref = held.at[chunk, c, block]
            start(
                near.remote(
                    ref,
                    ref,
                    send.at[chunk, index],
                    recv.at[chunk, block],
                    z if dz is None else z + dz,
                    1 - p if dp else p,
                    1 - q if dq else q,
                ),
                when,
            )

        def arrived(block):
            ref = held.at[chunk, c, block]
            near.remote(ref, ref, send.at[chunk, 0], recv.at[chunk, block], z, 1 - p, q).wait_recv()

        def both_ways(block, index):
            spread(block, index, dz=1, when=z < LEVELS - 1)
            spread(block, index + 1, dz=-1, when=z > 0)

        def onward(block, level, index):
            up = level < z
            spread(
                block,
                index,
                dz=jnp.where(up, 1, -1),
                when=jnp.where(up, z < LEVELS - 1, z > 0),
            )

        level = nearest(z, k)
        if kind == "own":
            own_copy(chunk).wait()
            block = near.block(z, p, q)
            if z_first:
                both_ways(block, 0)
                spread(block, 5, dp=1)
                spread(block, 9, dq=1)
            else:
                spread(block, 0, dp=1)
                both_ways(block, 1)
                spread(block, 11, dq=1)
        elif kind == "Z":
            block = near.block(level, p, q)
            arrived(block)
            if z_first:
                onward(block, level, 1 + k)
                spread(block, 5 + k, dp=1)
                spread(block, 9 + k, dq=1)
            else:
                onward(block, level, 2 + k)
                spread(block, 11 + k, dq=1)
        elif kind == "P":
            block = near.block(level, 1 - p, q)
            arrived(block)
            if z_first:
                spread(block, 13 + k, dq=1)
            else:
                both_ways(block, 6)
                spread(block, 15, dq=1)
        elif kind == "Y":
            block = near.block(level, 1 - p, q)
            arrived(block)
            onward(block, level, 7 + k)
            spread(block, 15 + k, dq=1)
        elif kind == "Q":
            for other in range(LEVELS):
                for side in range(2):
                    arrived(near.block(other, side, 1 - q))
            ref = held.at[chunk, c]
            start(sibling_copy(ref, ref, peer_send.at[chunk], peer_recv.at[chunk]))
        elif kind == "near":
            down_copy(chunk).wait()
            multiply(chunk, c)
        elif kind == "far":
            ref = held.at[chunk, 1 - c]
            sibling_copy(ref, ref, peer_send.at[chunk], peer_recv.at[chunk]).wait_recv()
            multiply(chunk, 1 - c)
            if chunk + 2 < CHUNKS:
                down_copy(chunk + 2).start()

    for chunk in range(CHUNKS):
        own_copy(chunk).start()
    down_copy(0).start()
    down_copy(1).start()
    for copy in saved_copies():
        copy.start()
    steps = listed(GATHER_ORDER, gather_names)
    ahead = [s for s in steps if s[1][0] == "own"][:AHEAD]
    for chunk, name in ahead:
        step(chunk, name)
    route(token_ref, router_ref, id_ref, probs_ref, gate_ref, letter)
    mail.post()
    met, part = False, 0
    for at, (chunk, name) in enumerate(steps):
        if (chunk, name) in ahead:
            continue
        if at % 5 == 0 and at > 10 and part < PARTS:
            if part == 0:
                for copy in saved_copies():
                    copy.wait()
            prepare(part)
            part += 1
        if name[0] == "near" and not met:
            mail.collect()
            count()
            met = True
        step(chunk, name)
    for turn, core in enumerate((c, 1 - c)):
        finish(core)
        for copy in grad_copies(core, turn):
            copy.start()
    met_ref[...] = inbox[...]
    for copy, when in started:
        if when is None:
            copy.wait_send()
        else:
            pl.when(when)(copy.wait_send)
    mail.close()
    for turn, core in enumerate((c, 1 - c)):
        for copy in grad_copies(core, turn):
            copy.wait()


def gather_call(grad, down_weight, tokens, router, ids, pre_gate, pre_up):
    rows, model_width = grad.shape
    hidden = down_weight.shape[0]
    devices = 2 * BLOCKS
    capacity = pre_gate.shape[0] // devices
    experts = router.shape[0]
    width = model_width // CHUNKS
    dma = pltpu.SemaphoreType.DMA
    vmem, anywhere = pl.BlockSpec(memory_space=pltpu.VMEM), pl.BlockSpec(memory_space=pl.ANY)
    halves = (2, BLOCKS, capacity, hidden)
    small = (devices, 8, rows)
    post = pltpu.VMEM(small, jnp.float32)
    blocked = (devices, capacity, hidden)
    return pl.pallas_call(
        gather_kernel,
        out_shape=(
            jax.ShapeDtypeStruct(halves, jnp.bfloat16),
            jax.ShapeDtypeStruct(halves, jnp.bfloat16),
            jax.ShapeDtypeStruct(small, jnp.float32),
            jax.ShapeDtypeStruct(small, jnp.float32),
            jax.ShapeDtypeStruct((experts, rows), jnp.float32),
            jax.ShapeDtypeStruct((experts, rows), jnp.float32),
        ),
        in_specs=[anywhere, anywhere, vmem, vmem, vmem, anywhere, anywhere],
        out_specs=(anywhere, anywhere, vmem, vmem, vmem, vmem),
        scratch_shapes=[
            pltpu.VMEM((CHUNKS, 2, BLOCKS, rows, width), jnp.bfloat16),
            pltpu.VMEM(halves, jnp.float32),
            pltpu.VMEM((BLOCKS, capacity, width), jnp.bfloat16),
            pltpu.VMEM((2, hidden, width), jnp.bfloat16),
            pltpu.VMEM((2, *blocked), jnp.bfloat16),
            pltpu.VMEM((2, *halves), jnp.bfloat16),
            post,
            post,
            dma((CHUNKS,)),
            dma((CHUNKS,)),
            dma((2,)),
            dma((2, 2)),
            dma((CHUNKS, 19)),
            dma((CHUNKS, BLOCKS)),
            dma((CHUNKS,)),
            dma((CHUNKS,)),
            dma((devices,)),
            dma((devices,)),
        ],
        compiler_params=pltpu.CompilerParams(
            has_side_effects=True, vmem_limit_bytes=62 * 2**20
        ),
        name="gather_upstream",
    )(
        grad,
        down_weight,
        tokens,
        router,
        ids,
        pre_gate.reshape(blocked),
        pre_up.reshape(blocked),
    )


def return_names(chunk):
    if RETURN_TYPES[chunk][0]:
        middle = [("P", k) for k in (3, 2, 1, 0)] + [("Z", k) for k in (3, 2, 1)]
    else:
        middle = [("Y", k) for k in (3, 2, 1)] + [("Z", k) for k in (3, 2, 1)] + [("P", 0)]
    leaves = [("leaf", (side, k)) for side in (1, 0) for k in (3, 2, 1, 0)]
    return [("away", 0), ("near", 0)] + leaves + middle + [("own", 0)]


def return_kernel(
    first_ref,
    second_ref,
    join_ref,
    gate_ref,
    up_ref,
    reply,
    probs_ref,
    share_ref,
    id_ref,
    aux_ref,
    token_ref,
    router_ref,
    out_ref,
    combine_ref,
    total_ref,
    held,
    landed,
    leaving,
    weights,
    weight_sem,
    send,
    recv,
    peer_send,
    peer_recv,
    answers,
    slope,
    outbox,
    inbox,
    reply_send,
    reply_recv,
    mail_send,
    mail_recv,
):
    z, x, y, c = place_of()
    replies = Mail(reply, answers, reply_send, reply_recv)
    mail = Mail(outbox, inbox, mail_send, mail_recv)
    tok_rows = token_ref.shape[0]
    experts = router_ref.shape[0]

    def route_back():
        probs, gates = probs_ref[...], share_ref[...]
        expert = lax.broadcasted_iota(jnp.int32, (experts, tok_rows), 0)
        picked = jnp.zeros((experts, tok_rows), jnp.float32)
        for k in range(id_ref.shape[0]):
            picked = picked + (id_ref[k : k + 1, :] == expert).astype(jnp.float32)
        chosen_sum = jnp.sum(probs * picked, axis=0, keepdims=True)
        combine = answers[:, 0, :]
        combine_ref[...] = combine
        mixed = jnp.sum(gates * combine, axis=0, keepdims=True)
        prob_grad = picked * (combine - mixed) / chosen_sum
        pairs = id_ref.shape[0] * tok_rows * 2 * LEVELS
        prob_grad = prob_grad + aux_ref[0] * (experts * answers[:, 1, :] / pairs)
        mean = jnp.sum(probs * prob_grad, axis=0, keepdims=True)
        logit_grad = probs * (prob_grad - mean)
        slope[...] = jnp.transpose(logit_grad).astype(jnp.bfloat16)
        part = token_ref.shape[1] // outbox.shape[0]

        @pl.loop(0, outbox.shape[0])
        def _(d):
            outbox[d] = jnp.dot(
                logit_grad.astype(jnp.bfloat16),
                token_ref[:, pl.ds(pl.multiple_of(d * part, part), part)],
                preferred_element_type=jnp.float32,
            ).astype(jnp.bfloat16)

    capacity = first_ref.shape[2]
    width = held.shape[-1]
    hidden = first_ref.shape[3]
    started = []

    def start(copy, when=None):
        if when is None:
            copy.start()
        else:
            pl.when(when)(copy.start)
        started.append((copy, when))

    def weight_copies(chunk):
        return [
            pltpu.make_async_copy(
                ref.at[pl.ds(chunk * width, width)],
                weights.at[chunk % 2, i],
                weight_sem.at[chunk, i],
            )
            for i, ref in enumerate((gate_ref, up_ref))
        ]

    def back_rows(chunk, core, store):
        group = 4

        @pl.loop(0, BLOCKS // group)
        def _(i):
            total = None
            for j, ref in enumerate((first_ref, second_ref)):
                term = lax.dot_general(
                    ref[core, pl.ds(i * group, group)].reshape(-1, hidden),
                    weights[chunk % 2, j],
                    (((1,), (1,)), ((), ())),
                    preferred_element_type=jnp.float32,
                )
                total = term if total is None else total + term
            store(i * group, group, total.astype(jnp.bfloat16).reshape(group, capacity, width))

    def leave(chunk):
        return sibling_copy(
            leaving.at[chunk % 2],
            held.at[chunk, :, pl.ds(capacity, capacity)],
            peer_send.at[chunk],
            peer_recv.at[chunk],
        )

    def step(chunk, name):
        kind, k = name
        z_first, swap = RETURN_TYPES[chunk]
        near = Copies(swap)
        p, q = near.p, near.q

        def give(block, slot, index, dz=None, dp=0, dq=0, when=None):
            start(
                near.remote(
                    held.at[chunk, block],
                    landed.at[chunk, slot],
                    send.at[chunk, index],
                    recv.at[chunk, slot],
                    z if dz is None else z + dz,
                    1 - p if dp else p,
                    1 - q if dq else q,
                ),
                when,
            )

        def take(block, slot):
            ref = landed.at[chunk, slot]
            near.remote(ref, ref, send.at[chunk, 0], recv.at[chunk, slot], z, 1 - p, q).wait_recv()
            held[chunk, block] = (
                held[chunk, block].astype(jnp.float32) + landed[chunk, slot].astype(jnp.float32)
            ).astype(jnp.bfloat16)

        def take_outer(block, level, base):
            pl.when(jnp.where(level > z, z > 0, z < LEVELS - 1))(lambda: take(block, base + level))

        def give_inner(block, level, base, index):
            up = level > z
            last = level == z - 1
            give(
                block,
                base + jnp.where(last, LEVELS, level),
                index,
                dz=jnp.where(up, 1, -1),
            )

        def take_ends(block, base):
            pl.when(z > 0)(lambda: take(block, base + z))
            pl.when(z < LEVELS - 1)(lambda: take(block, base + LEVELS))

        level = None if kind == "leaf" else nearest(z, k)
        if kind == "away":
            for copy in weight_copies(chunk):
                copy.wait()
            if chunk >= 2:
                leave(chunk - 2).wait_send()

            def store(at, count, value):
                leaving[chunk % 2, pl.ds(at, count)] = value

            back_rows(chunk, 1 - c, store)
            leave(chunk).start()
        elif kind == "near":

            def store(at, count, value):
                held[chunk, pl.ds(at, count), pl.ds(0, capacity)] = value

            back_rows(chunk, c, store)
            if chunk + 2 < CHUNKS:
                for copy in weight_copies(chunk + 2):
                    copy.start()
            leave(chunk).wait_recv()

            @pl.loop(0, BLOCKS, unroll=4)
            def _(b):
                held[chunk, b] = jnp.dot(
                    join_ref[b], held[chunk, b], preferred_element_type=jnp.float32
                ).astype(jnp.bfloat16)
        elif kind == "leaf":
            side, far = k
            level = nearest(z, far)
            column = 1 - p if side else p
            give(near.block(level, column, 1 - q), level * 2 + column, far * 2 + side, dq=1)
        elif kind == "P" and z_first:
            block = near.block(level, 1 - p, q)
            take(block, level * 2 + 1 - p)
            give(block, 8 + level, 8 + k, dp=1)
        elif kind == "P":
            block = near.block(z, 1 - p, q)
            take(block, z * 2 + 1 - p)
            take_ends(block, 13)
            give(block, 18, 14, dp=1)
        elif kind == "Z":
            block = near.block(level, p, q)
            take(block, level * 2 + p)
            if z_first:
                take(block, 8 + level)
                take_outer(block, level, 12)
                give_inner(block, level, 12, 11 + k)
            else:
                take_outer(block, level, 8)
                give_inner(block, level, 8, 7 + k)
        elif kind == "Y":
            block = near.block(level, 1 - p, q)
            take(block, level * 2 + 1 - p)
            take_outer(block, level, 13)
            give_inner(block, level, 13, 10 + k)
        elif kind == "own":
            block = near.block(z, p, q)
            take(block, z * 2 + p)
            if z_first:
                take(block, 8 + z)
                take_ends(block, 12)
            else:
                take_ends(block, 8)
                take(block, 18)
            here = slice(chunk * width, (chunk + 1) * width)
            routed = jnp.dot(slope[...], router_ref[:, here], preferred_element_type=jnp.float32)
            out_ref[:, here] = (held[chunk, block].astype(jnp.float32) + routed).astype(jnp.bfloat16)

    for chunk in range(2):
        for copy in weight_copies(chunk):
            copy.start()
    replies.post()
    begun = False
    for chunk, name in listed(RETURN_ORDER, return_names):
        step(chunk, name)
        if not begun:
            begun = True
            replies.collect()
            route_back()
            mail.post()
    mail.collect()
    total_ref[...] = jnp.sum(inbox[...].astype(jnp.float32), axis=0)
    replies.close()
    mail.close()
    for chunk in range(CHUNKS - 2, CHUNKS):
        leave(chunk).wait_send()
    for copy, when in started:
        if when is None:
            copy.wait_send()
        else:
            pl.when(when)(copy.wait_send)


def return_call(
    first, second, joined, gate_weight, up_weight, reply, probs, shares, ids, aux, tokens, router
):
    model_width, hidden = gate_weight.shape
    capacity = first.shape[2]
    rows = joined.shape[1]
    experts, devices = router.shape[0], reply.shape[0]
    width = model_width // CHUNKS
    dma = pltpu.SemaphoreType.DMA
    vmem, anywhere = pl.BlockSpec(memory_space=pltpu.VMEM), pl.BlockSpec(memory_space=pl.ANY)
    post = pltpu.VMEM((devices, experts, model_width // devices), jnp.bfloat16)
    return pl.pallas_call(
        return_kernel,
        out_shape=(
            jax.ShapeDtypeStruct((rows, model_width), jnp.bfloat16),
            jax.ShapeDtypeStruct((experts, rows), jnp.float32),
            jax.ShapeDtypeStruct((experts, model_width // devices), jnp.float32),
        ),
        in_specs=[vmem, vmem, vmem, anywhere, anywhere]
        + [vmem] * 4
        + [pl.BlockSpec(memory_space=pltpu.SMEM), vmem, vmem],
        out_specs=(vmem, vmem, vmem),
        scratch_shapes=[
            pltpu.VMEM((CHUNKS, BLOCKS, rows, width), jnp.bfloat16),
            pltpu.VMEM((CHUNKS, 19, rows, width), jnp.bfloat16),
            pltpu.VMEM((2, BLOCKS, capacity, width), jnp.bfloat16),
            pltpu.VMEM((2, 2, width, hidden), jnp.bfloat16),
            dma((CHUNKS, 2)),
            dma((CHUNKS, 15)),
            dma((CHUNKS, 19)),
            dma((CHUNKS,)),
            dma((CHUNKS,)),
            pltpu.VMEM(reply.shape, jnp.float32),
            pltpu.VMEM((rows, experts), jnp.bfloat16),
            post,
            post,
            dma((devices,)),
            dma((devices,)),
            dma((devices,)),
            dma((devices,)),
        ],
        compiler_params=pltpu.CompilerParams(
            has_side_effects=True, vmem_limit_bytes=60 * 2**20
        ),
        name="back_return",
    )(first, second, joined, gate_weight, up_weight, reply, probs, shares, ids, aux, tokens, router)


def gathered_shards(
    tokens,
    out_grad,
    router_weight,
    gate_weight,
    up_weight,
    down_weight,
    saved_gate,
    saved_up,
    expert_ids,
    aux_weight,
):
    inputs = tokens[0]
    chosen_ids = expert_ids[0]
    tok_rows = chosen_ids.shape[0]
    experts = router_weight.shape[1]
    devices = lax.axis_size("seq") * lax.axis_size("exp")
    capacity = saved_gate.shape[1] // devices
    router, ids = router_weight.T, chosen_ids.T

    grad_first, grad_second, met, reply, router_probs, gate_dense = gather_call(
        out_grad[0], down_weight[0], inputs, router, ids, saved_gate[0], saved_up[0]
    )

    here_core = lax.axis_index("exp") % 2
    met = lax.dynamic_index_in_dim(
        met.reshape((devices // 2, 2) + met.shape[1:]), here_core, 1, keepdims=False
    )
    join_pos = jnp.concatenate(
        [
            jnp.broadcast_to(met[:, i, :, None], (devices // 2, tok_rows, capacity))
            for i in (0, 2)
        ],
        axis=2,
    ).astype(jnp.int32)
    joined = (join_pos == jnp.arange(2 * capacity, dtype=jnp.int32) % capacity).astype(jnp.bfloat16)

    token_grad, combine_dense, router_grad = return_call(
        grad_first,
        grad_second,
        joined,
        gate_weight[0],
        up_weight[0],
        reply,
        router_probs,
        gate_dense,
        ids,
        aux_weight,
        inputs,
        router,
    )
    onehot = chosen_ids[:, None, :] == jnp.arange(experts, dtype=jnp.int32)[:, None]
    combine_grad = jnp.sum(jnp.where(onehot, combine_dense.T[:, :, None], 0.0), axis=1)
    return (token_grad[None], combine_grad[None], router_grad.T)


def program(*arrays):
    tok_rows = arrays[0].shape[1]
    seq_size, exp_size = lax.axis_size("seq"), lax.axis_size("exp")
    slots = arrays[6].shape[1]
    lined = exp_size == 4 and seq_size == 2 * LEVELS
    fits = arrays[0].shape[2] == 4096 and arrays[6].shape[2] == 768 and tok_rows == 128
    if lined and fits and seq_size * exp_size * tok_rows <= 2 * slots:
        return gathered_shards(*arrays)
    return shards(*arrays)


def solution(mesh):
    placed = (
        P("exp", "seq", None),
        P("exp", "seq", None),
        P(),
        P(("seq", "exp"), None, None),
        P(("seq", "exp"), None, None),
        P(("seq", "exp"), None, None),
        P(("seq", "exp"), None, None),
        P(("seq", "exp"), None, None),
        P("exp", "seq", None),
        P(),
    )
    return jax.shard_map(
        program,
        mesh=mesh,
        in_specs=placed,
        out_specs=(P("exp", "seq", None), P("exp", "seq", None), P(("seq", "exp"), None)),
        check_vma=False,
    )
```

```python
import jax
import jax.numpy as jnp
from jax import lax
from jax.experimental import pallas as pl
from jax.experimental.pallas import tpu as pltpu
from jax.sharding import PartitionSpec as P


def expert_backward(grad_rows, gate_rows, w_gate, w_up, w_down, pre_gate, pre_up):
    upstream = jnp.einsum("rd,fd->rf", grad_rows, w_down, preferred_element_type=jnp.float32)
    first = pre_gate.astype(jnp.float32)
    second = pre_up.astype(jnp.float32)
    gate_sig = jax.nn.sigmoid(first)
    gate_act = first * gate_sig
    hidden = gate_act * second
    slot_combine = jnp.sum(upstream * hidden, axis=-1).astype(jnp.bfloat16)
    scaled = gate_rows.astype(jnp.float32)[:, None] * upstream
    grad_first = (scaled * second * gate_sig * (1.0 + first * (1.0 - gate_sig))).astype(
        jnp.bfloat16
    )
    grad_second = (scaled * gate_act).astype(jnp.bfloat16)
    back_rows = jnp.einsum("rf,df->rd", grad_first, w_gate, preferred_element_type=jnp.float32)
    back_rows = back_rows + jnp.einsum(
        "rf,df->rd", grad_second, w_up, preferred_element_type=jnp.float32
    )
    return (back_rows.astype(jnp.bfloat16), slot_combine)


def shards(
    tokens,
    out_grad,
    router_weight,
    gate_weight,
    up_weight,
    down_weight,
    saved_gate,
    saved_up,
    expert_ids,
    aux_weight,
):
    seq_size = lax.axis_size("seq")
    exp_size = lax.axis_size("exp")
    devices = seq_size * exp_size
    inputs = tokens[0]
    upstream_grad = out_grad[0]
    chosen_ids = expert_ids[0]
    tok_rows, top_count = chosen_ids.shape
    model_width = inputs.shape[1]
    experts = router_weight.shape[1]
    capacity = saved_gate.shape[1] // devices
    logits = jnp.dot(inputs, router_weight, preferred_element_type=jnp.float32)
    router_probs = jax.nn.softmax(logits, axis=-1)
    chosen = jnp.take_along_axis(router_probs, chosen_ids, axis=1)
    chosen_sum = jnp.sum(chosen, axis=1, keepdims=True)
    gate_vals = chosen / chosen_sum
    onehot = (
        chosen_ids.reshape(-1)[:, None] == jnp.arange(experts, dtype=jnp.int32)[None, :]
    ).astype(jnp.int32)
    rank_before = jnp.cumsum(onehot, axis=0) - onehot
    slot_pos = jnp.sum(rank_before * onehot, axis=1)
    slot_index = chosen_ids.reshape(-1) * capacity + slot_pos
    token_order = jnp.arange(tok_rows * top_count, dtype=jnp.int32) // top_count
    slot_token = (
        jnp.full((experts * capacity,), tok_rows, jnp.int32).at[slot_index].set(token_order)
    )
    grad_padded = jnp.concatenate(
        [upstream_grad, jnp.zeros((1, model_width), jnp.bfloat16)], axis=0
    )
    grad_slots = grad_padded[slot_token]
    gate_slots = (
        jnp.zeros((experts * capacity,), jnp.bfloat16)
        .at[slot_index]
        .set(gate_vals.reshape(-1).astype(jnp.bfloat16))
    )
    chosen_count = jnp.sum(onehot.reshape(tok_rows, top_count, experts), axis=1).astype(jnp.float32)
    local_counts = jnp.sum(chosen_count, axis=0)
    seq_counts = lax.psum(local_counts, "seq")
    recv_grad, recv_gate = (
        lax.all_to_all(
            grad_slots.reshape(experts, 1, capacity, model_width),
            ("seq", "exp"),
            split_axis=0,
            concat_axis=1,
            tiled=True,
        ),
        lax.all_to_all(
            gate_slots.reshape(experts, 1, capacity),
            ("seq", "exp"),
            split_axis=0,
            concat_axis=1,
            tiled=True,
        ),
    )
    back_rows, slot_combine = expert_backward(
        recv_grad.reshape(-1, model_width),
        recv_gate.reshape(-1),
        gate_weight[0],
        up_weight[0],
        down_weight[0],
        saved_gate[0],
        saved_up[0],
    )
    returned, combine_back = (
        lax.all_to_all(
            back_rows.reshape(1, devices, capacity, model_width),
            ("seq", "exp"),
            split_axis=1,
            concat_axis=0,
            tiled=True,
        ),
        lax.all_to_all(
            slot_combine.reshape(1, devices, capacity),
            ("seq", "exp"),
            split_axis=1,
            concat_axis=0,
            tiled=True,
        ),
    )
    returned_rows = returned.reshape(experts * capacity, model_width)
    expert_sum = jnp.sum(
        returned_rows[slot_index].reshape(tok_rows, top_count, model_width).astype(jnp.float32),
        axis=1,
    )
    combine_grad = (
        combine_back.reshape(-1)[slot_index].reshape(tok_rows, top_count).astype(jnp.float32)
    )
    prob_sel = (
        combine_grad - jnp.sum(gate_vals * combine_grad, axis=1, keepdims=True)
    ) / chosen_sum
    prob_grad = jnp.einsum(
        "tk,tke->te", prob_sel, onehot.reshape(tok_rows, top_count, experts).astype(jnp.float32)
    )
    fraction = experts * seq_counts / (top_count * tok_rows * seq_size)
    prob_grad = prob_grad + aux_weight[0] * fraction[None, :]
    dlogits = router_probs * (prob_grad - jnp.sum(router_probs * prob_grad, axis=1, keepdims=True))
    logit_grad = dlogits.astype(jnp.bfloat16)
    token_grad = expert_sum + jnp.einsum(
        "te,de->td", logit_grad, router_weight, preferred_element_type=jnp.float32
    )
    router_grad = lax.psum_scatter(
        jnp.einsum("td,te->de", inputs, logit_grad, preferred_element_type=jnp.float32),
        ("seq", "exp"),
        scatter_dimension=0,
        tiled=True,
    )
    return (token_grad.astype(jnp.bfloat16)[None], combine_grad[None], router_grad)

MESH = pl.DeviceIdType.MESH
GATHER_TYPES = ((False, False), (False, True), (True, False), (False, True), (False, False), (True, True), (False, True), (False, False))
RETURN_TYPES = ((False, False), (False, True), (False, False), (False, True), (True, True), (True, False), (False, True), (False, False))
GATHER_ORDER = (
    60, 40, 80, 100, 20, 0, 101, 42, 41, 120, 22, 44, 21, 2, 102, 1, 23, 121, 140, 61, 43, 3, 24, 6,
    7, 5, 26, 25, 45, 81, 106, 62, 47, 4, 63, 103, 46, 65, 27, 85, 104, 8, 66, 142, 9, 86, 107, 83,
    82, 10, 28, 122, 64, 29, 84, 67, 125, 123, 105, 143, 48, 30, 87, 68, 141, 49, 69, 126, 50, 124,
    145, 88, 70, 89, 108, 146, 127, 109, 144, 90, 128, 147, 110, 129, 148, 149, 130, 150,
)
RETURN_ORDER = (
    0, 20, 1, 2, 3, 21, 22, 10, 27, 4, 26, 40, 6, 11, 23, 8, 28, 60, 12, 30, 41, 42, 13, 61, 67, 62,
    46, 33, 80, 50, 47, 100, 43, 45, 7, 5, 53, 24, 81, 31, 63, 120, 51, 82, 64, 34, 101, 140, 68,
    103, 48, 32, 85, 83, 54, 106, 107, 44, 70, 66, 121, 141, 105, 55, 146, 35, 108, 90, 124, 123,
    122, 14, 93, 73, 144, 128, 25, 84, 15, 130, 126, 102, 109, 86, 142, 74, 125, 127, 143, 36, 132,
    104, 72, 129, 65, 71, 9, 92, 29, 153, 110, 131, 52, 145, 113, 150, 56, 16, 151, 49, 111, 133,
    75, 112, 94, 88, 114, 76, 152, 87, 148, 91, 147, 57, 115, 136, 89, 149, 134, 69, 135, 37, 116,
    95, 156, 154, 96, 155, 117, 137, 17, 97, 77, 157,
)

CHUNKS = len(GATHER_TYPES)
LEVELS = 4
AHEAD = 3
PARTS = 4
BLOCKS = 4 * LEVELS


def place_of():
    seq, exp = lax.axis_index("seq"), lax.axis_index("exp")
    return seq // 2, seq % 2, exp // 2, exp % 2


def nearest(z, k):
    table = ((0, 1, 2, 3), (1, 2, 0, 3), (2, 1, 3, 0), (3, 2, 1, 0))
    value = jnp.int32(table[3][k])
    for level in (2, 1, 0):
        value = jnp.where(z == level, jnp.int32(table[level][k]), value)
    return value


def planar(first, second, swap):
    return (second, first) if swap else (first, second)


class Copies:
    def __init__(self, swap):
        self.z, self.x, self.y, self.c = place_of()
        self.swap = swap
        self.p, self.q = planar(self.x, self.y, swap)

    def block(self, z, p, q):
        x, y = planar(p, q, self.swap)
        return (z * 2 + x) * 2 + y

    def device(self, z, p, q):
        x, y = planar(p, q, self.swap)
        return z * 2 + x, y * 2 + self.c

    def remote(self, src, dst, send, recv, z, p, q):
        return pltpu.make_async_remote_copy(
            src_ref=src,
            dst_ref=dst,
            send_sem=send,
            recv_sem=recv,
            device_id=self.device(z, p, q),
            device_id_type=MESH,
        )


def sibling_copy(src, dst, send, recv):
    z, x, y, c = place_of()
    return pltpu.make_async_remote_copy(
        src_ref=src,
        dst_ref=dst,
        send_sem=send,
        recv_sem=recv,
        device_id=(z * 2 + x, y * 2 + 1 - c),
        device_id_type=MESH,
    )


def gather_names(chunk):
    if GATHER_TYPES[chunk][0]:
        middle = [("Z", k) for k in (1, 2, 3)] + [("P", k) for k in range(4)]
    else:
        middle = [("P", 0)] + [("Z", k) for k in (1, 2, 3)] + [("Y", k) for k in (1, 2, 3)]
    return [("own", 0)] + middle + [("Q", 0), ("near", 0), ("far", 0)]


def listed(order, names):
    return [(code // 20, names(code // 20)[code % 20]) for code in order]


def route(token_ref, router_ref, id_ref, probs_ref, gate_ref, letter):
    experts, rows = probs_ref.shape
    logits = lax.dot_general(
        router_ref[...], token_ref[...], (((1,), (1,)), ((), ())), preferred_element_type=jnp.float32
    )
    shifted = jnp.exp(logits - jnp.max(logits, axis=0, keepdims=True))
    probs = shifted / jnp.sum(shifted, axis=0, keepdims=True)
    expert = lax.broadcasted_iota(jnp.int32, (experts, rows), 0)
    picked = jnp.zeros((experts, rows), jnp.float32)
    for k in range(id_ref.shape[0]):
        picked = picked + (id_ref[k : k + 1, :] == expert).astype(jnp.float32)
    chosen = probs * picked
    gates = chosen / jnp.sum(chosen, axis=0, keepdims=True)
    earlier = lax.broadcasted_iota(jnp.int32, (rows, rows), 0)
    earlier = (earlier < lax.broadcasted_iota(jnp.int32, (rows, rows), 1)).astype(jnp.float32)
    rank = jnp.dot(
        picked.astype(jnp.bfloat16),
        earlier.astype(jnp.bfloat16),
        preferred_element_type=jnp.float32,
    )
    slot_pos = jnp.where(picked > 0, rank, -1.0)
    sent_gates = gates.astype(jnp.bfloat16).astype(jnp.float32)
    probs_ref[...] = probs
    gate_ref[...] = gates
    for e in range(experts):
        letter[e, 0:1, :] = slot_pos[e : e + 1, :]
        letter[e, 1:2, :] = sent_gates[e : e + 1, :]
        letter[e, 2:3, :] = slot_pos[e ^ 1 : (e ^ 1) + 1, :]


class Mail:
    def __init__(self, outbox, inbox, send, recv):
        z, x, y, c = place_of()
        self.me = (z * 2 + x) * 4 + y * 2 + c
        self.outbox, self.inbox, self.send, self.recv = outbox, inbox, send, recv
        self.devices = outbox.shape[0]

    def copies(self):
        for step in range(1, self.devices):
            to = (self.me + step) % self.devices
            yield pltpu.make_async_remote_copy(
                src_ref=self.outbox.at[to],
                dst_ref=self.inbox.at[self.me],
                send_sem=self.send.at[step],
                recv_sem=self.recv.at[step],
                device_id=(to // 4, to % 4),
                device_id_type=MESH,
            )

    def post(self):
        self.inbox[self.me] = self.outbox[self.me]
        for copy in self.copies():
            copy.start()

    def collect(self):
        for step in range(1, self.devices):
            ref = self.inbox.at[(self.me - step + self.devices) % self.devices]
            pltpu.make_async_remote_copy(
                src_ref=ref,
                dst_ref=ref,
                send_sem=self.send.at[step],
                recv_sem=self.recv.at[step],
                device_id=(self.me // 4, self.me % 4),
                device_id_type=MESH,
            ).wait_recv()

    def close(self):
        for copy in self.copies():
            copy.wait_send()


def gather_kernel(
    grad_ref,
    down_ref,
    token_ref,
    router_ref,
    id_ref,
    pre_gate_ref,
    pre_up_ref,
    first_ref,
    second_ref,
    join_ref,
    reply,
    probs_ref,
    gate_ref,
    held,
    up_ref,
    rows,
    down,
    saved,
    grads,
    letter,
    inbox,
    own_sem,
    down_sem,
    saved_sem,
    grads_sem,
    send,
    recv,
    peer_send,
    peer_recv,
    mail_send,
    mail_recv,
):
    z, x, y, c = place_of()
    width = held.shape[-1]
    capacity = rows.shape[1]
    tok_rows = held.shape[-2]
    here = (z * 2 + x) * 2 + y
    started = []
    mail = Mail(letter, inbox, mail_send, mail_recv)

    def spots(core, b):
        slot = lax.broadcasted_iota(jnp.int32, (capacity, tok_rows), 0).astype(jnp.float32)
        return inbox[b * 2 + core, 0:1, :] == slot

    def saved_copies():
        return [
            pltpu.make_async_copy(ref, saved.at[i], saved_sem.at[i])
            for i, ref in enumerate((pre_gate_ref, pre_up_ref))
        ]

    def grad_copies(core, turn):
        return [
            pltpu.make_async_copy(grads.at[i, core], ref.at[core], grads_sem.at[turn, i])
            for i, ref in enumerate((first_ref, second_ref))
        ]

    def count():
        sources = inbox.shape[0]
        taken = (inbox[:, 0, :] >= 0).astype(jnp.bfloat16)
        one = lax.broadcasted_iota(jnp.int32, (sources, sources), 0) % 4
        two = lax.broadcasted_iota(jnp.int32, (sources, sources), 1) % 4
        alike = (one == two).astype(jnp.float32).astype(jnp.bfloat16)
        total = jnp.dot(alike, taken, preferred_element_type=jnp.float32)
        total = jnp.broadcast_to(jnp.sum(total, axis=1, keepdims=True), total.shape)
        for s in range(sources):
            reply[s, 1:2, :] = total[s : s + 1, :]

    def join():
        slot = lax.broadcasted_iota(jnp.int32, (capacity, tok_rows), 0).astype(jnp.float32)

        @pl.loop(0, BLOCKS)
        def _(b):
            both = [
                (inbox[b * 2 + c, row : row + 1, :] == slot).astype(jnp.float32) for row in (0, 2)
            ]
            join_ref[b] = jnp.transpose(jnp.concatenate(both, axis=0)).astype(jnp.bfloat16)

    def prepare(part):
        @pl.loop(part * BLOCKS // PARTS, (part + 1) * BLOCKS // PARTS)
        def _(b):
            for core in range(2):
                first = saved[0, b * 2 + core].astype(jnp.float32)
                second = saved[1, b * 2 + core].astype(jnp.float32)
                sig = jax.nn.sigmoid(first)
                grads[0, core, b] = (second * sig * (1.0 + first * (1.0 - sig))).astype(jnp.bfloat16)
                grads[1, core, b] = (first * sig).astype(jnp.bfloat16)

    def finish(core):
        @pl.loop(0, BLOCKS)
        def _(b):
            source = b * 2 + core
            upstream = up_ref[core, b]
            act = grads[1, core, b].astype(jnp.float32)
            at = spots(core, b)
            gate = jnp.sum(jnp.where(at, inbox[source, 1:2, :], 0.0), axis=1, keepdims=True)
            hidden = act * saved[1, source].astype(jnp.float32)
            combine = jnp.sum(upstream * hidden, axis=1, keepdims=True)
            combine = combine.astype(jnp.bfloat16).astype(jnp.float32)
            reply[source, 0:1, :] = jnp.sum(jnp.where(at, combine, 0.0), axis=0, keepdims=True)
            scaled = gate * upstream
            grads[0, core, b] = (scaled * grads[0, core, b].astype(jnp.float32)).astype(jnp.bfloat16)
            grads[1, core, b] = (scaled * act).astype(jnp.bfloat16)

    def start(copy, when=None):
        if when is None:
            copy.start()
        else:
            pl.when(when)(copy.start)
        started.append((copy, when))

    def over(chunk, core, turn):
        level = nearest(z, turn)
        ref = held.at[chunk, core, pl.ds(level * 4, 4)]
        return sibling_copy(ref, ref, peer_send.at[chunk, turn], peer_recv.at[chunk, turn])

    def own_copy(chunk):
        return pltpu.make_async_copy(
            grad_ref.at[:, pl.ds(chunk * width, width)], held.at[chunk, c, here], own_sem.at[chunk]
        )

    def down_copy(chunk):
        return pltpu.make_async_copy(
            down_ref.at[:, pl.ds(chunk * width, width)], down.at[chunk % 2], down_sem.at[chunk]
        )

    def multiply(chunk, core):
        @pl.loop(0, BLOCKS, unroll=4)
        def _(b):
            rows[b] = jnp.dot(
                spots(core, b).astype(jnp.float32).astype(jnp.bfloat16),
                held[chunk, core, b],
                preferred_element_type=jnp.float32,
            ).astype(jnp.bfloat16)

        group = 4

        @pl.loop(0, BLOCKS // group)
        def _(i):
            picked = rows[pl.ds(i * group, group)]
            term = lax.dot_general(
                picked.reshape(-1, width),
                down[chunk % 2],
                (((1,), (1,)), ((), ())),
                preferred_element_type=jnp.float32,
            ).reshape(group, -1, down.shape[1])
            if chunk == 0:
                up_ref[core, pl.ds(i * group, group)] = term
            else:
                up_ref[core, pl.ds(i * group, group)] += term

    def step(chunk, name):
        kind, k = name
        z_first, swap = GATHER_TYPES[chunk]
        near = Copies(swap)
        p, q = near.p, near.q

        def spread(block, index, dz=None, dp=0, dq=0, when=None):
            ref = held.at[chunk, c, block]
            start(
                near.remote(
                    ref,
                    ref,
                    send.at[chunk, index],
                    recv.at[chunk, block],
                    z if dz is None else z + dz,
                    1 - p if dp else p,
                    1 - q if dq else q,
                ),
                when,
            )

        def arrived(block):
            ref = held.at[chunk, c, block]
            near.remote(ref, ref, send.at[chunk, 0], recv.at[chunk, block], z, 1 - p, q).wait_recv()

        def both_ways(block, index):
            spread(block, index, dz=1, when=z < LEVELS - 1)
            spread(block, index + 1, dz=-1, when=z > 0)

        def onward(block, level, index):
            up = level < z
            spread(
                block,
                index,
                dz=jnp.where(up, 1, -1),
                when=jnp.where(up, z < LEVELS - 1, z > 0),
            )

        level = nearest(z, k)
        if kind == "own":
            own_copy(chunk).wait()
            block = near.block(z, p, q)
            if z_first:
                both_ways(block, 0)
                spread(block, 5, dp=1)
                spread(block, 9, dq=1)
            else:
                spread(block, 0, dp=1)
                both_ways(block, 1)
                spread(block, 11, dq=1)
        elif kind == "Z":
            block = near.block(level, p, q)
            arrived(block)
            if z_first:
                onward(block, level, 1 + k)
                spread(block, 5 + k, dp=1)
                spread(block, 9 + k, dq=1)
            else:
                onward(block, level, 2 + k)
                spread(block, 11 + k, dq=1)
        elif kind == "P":
            block = near.block(level, 1 - p, q)
            arrived(block)
            if z_first:
                spread(block, 13 + k, dq=1)
            else:
                both_ways(block, 6)
                spread(block, 15, dq=1)
        elif kind == "Y":
            block = near.block(level, 1 - p, q)
            arrived(block)
            onward(block, level, 7 + k)
            spread(block, 15 + k, dq=1)
        elif kind == "Q":
            for turn in range(LEVELS):
                for side in range(2):
                    arrived(near.block(nearest(z, turn), side, 1 - q))
                start(over(chunk, c, turn))
        elif kind == "near":
            down_copy(chunk).wait()
            multiply(chunk, c)
        elif kind == "far":
            for turn in range(LEVELS):
                over(chunk, 1 - c, turn).wait_recv()
            multiply(chunk, 1 - c)
            if chunk + 2 < CHUNKS:
                down_copy(chunk + 2).start()

    for chunk in range(CHUNKS):
        own_copy(chunk).start()
    down_copy(0).start()
    down_copy(1).start()
    for copy in saved_copies():
        copy.start()
    steps = listed(GATHER_ORDER, gather_names)
    ahead = [s for s in steps if s[1][0] == "own"][:AHEAD]
    for chunk, name in ahead:
        step(chunk, name)
    route(token_ref, router_ref, id_ref, probs_ref, gate_ref, letter)
    mail.post()
    met, part = False, 0
    for at, (chunk, name) in enumerate(steps):
        if (chunk, name) in ahead:
            continue
        if at % 5 == 0 and at > 10 and part < PARTS:
            if part == 0:
                for copy in saved_copies():
                    copy.wait()
            prepare(part)
            part += 1
        if name[0] == "near" and not met:
            mail.collect()
            count()
            join()
            met = True
        step(chunk, name)
    for turn, core in enumerate((c, 1 - c)):
        finish(core)
        for copy in grad_copies(core, turn):
            copy.start()
    for copy, when in started:
        if when is None:
            copy.wait_send()
        else:
            pl.when(when)(copy.wait_send)
    mail.close()
    for turn, core in enumerate((c, 1 - c)):
        for copy in grad_copies(core, turn):
            copy.wait()


def gather_call(grad, down_weight, tokens, router, ids, pre_gate, pre_up):
    rows, model_width = grad.shape
    hidden = down_weight.shape[0]
    devices = 2 * BLOCKS
    capacity = pre_gate.shape[0] // devices
    experts = router.shape[0]
    width = model_width // CHUNKS
    dma = pltpu.SemaphoreType.DMA
    vmem, anywhere = pl.BlockSpec(memory_space=pltpu.VMEM), pl.BlockSpec(memory_space=pl.ANY)
    halves = (2, BLOCKS, capacity, hidden)
    small = (devices, 8, rows)
    post = pltpu.VMEM(small, jnp.float32)
    blocked = (devices, capacity, hidden)
    return pl.pallas_call(
        gather_kernel,
        out_shape=(
            jax.ShapeDtypeStruct(halves, jnp.bfloat16),
            jax.ShapeDtypeStruct(halves, jnp.bfloat16),
            jax.ShapeDtypeStruct((BLOCKS, rows, 2 * capacity), jnp.bfloat16),
            jax.ShapeDtypeStruct(small, jnp.float32),
            jax.ShapeDtypeStruct((experts, rows), jnp.float32),
            jax.ShapeDtypeStruct((experts, rows), jnp.float32),
        ),
        in_specs=[anywhere, anywhere, vmem, vmem, vmem, anywhere, anywhere],
        out_specs=(anywhere, anywhere, vmem, vmem, vmem, vmem),
        scratch_shapes=[
            pltpu.VMEM((CHUNKS, 2, BLOCKS, rows, width), jnp.bfloat16),
            pltpu.VMEM(halves, jnp.float32),
            pltpu.VMEM((BLOCKS, capacity, width), jnp.bfloat16),
            pltpu.VMEM((2, hidden, width), jnp.bfloat16),
            pltpu.VMEM((2, *blocked), jnp.bfloat16),
            pltpu.VMEM((2, *halves), jnp.bfloat16),
            post,
            post,
            dma((CHUNKS,)),
            dma((CHUNKS,)),
            dma((2,)),
            dma((2, 2)),
            dma((CHUNKS, 19)),
            dma((CHUNKS, BLOCKS)),
            dma((CHUNKS, LEVELS)),
            dma((CHUNKS, LEVELS)),
            dma((devices,)),
            dma((devices,)),
        ],
        compiler_params=pltpu.CompilerParams(
            has_side_effects=True, vmem_limit_bytes=62 * 2**20
        ),
        name="gather_upstream",
    )(
        grad,
        down_weight,
        tokens,
        router,
        ids,
        pre_gate.reshape(blocked),
        pre_up.reshape(blocked),
    )


def return_names(chunk):
    if RETURN_TYPES[chunk][0]:
        middle = [("P", k) for k in (3, 2, 1, 0)] + [("Z", k) for k in (3, 2, 1)]
    else:
        middle = [("Y", k) for k in (3, 2, 1)] + [("Z", k) for k in (3, 2, 1)] + [("P", 0)]
    leaves = [("leaf", (side, k)) for side in (1, 0) for k in (3, 2, 1, 0)]
    return [("away", 0), ("near", 0)] + leaves + middle + [("own", 0)]


def return_kernel(
    first_ref,
    second_ref,
    join_ref,
    gate_ref,
    up_ref,
    reply,
    probs_ref,
    share_ref,
    id_ref,
    aux_ref,
    token_ref,
    router_ref,
    out_ref,
    combine_ref,
    total_ref,
    held,
    landed,
    leaving,
    weights,
    weight_sem,
    send,
    recv,
    peer_send,
    peer_recv,
    answers,
    slope,
    outbox,
    inbox,
    reply_send,
    reply_recv,
    mail_send,
    mail_recv,
):
    z, x, y, c = place_of()
    replies = Mail(reply, answers, reply_send, reply_recv)
    mail = Mail(outbox, inbox, mail_send, mail_recv)
    tok_rows = token_ref.shape[0]
    experts = router_ref.shape[0]

    def route_back():
        probs, gates = probs_ref[...], share_ref[...]
        expert = lax.broadcasted_iota(jnp.int32, (experts, tok_rows), 0)
        picked = jnp.zeros((experts, tok_rows), jnp.float32)
        for k in range(id_ref.shape[0]):
            picked = picked + (id_ref[k : k + 1, :] == expert).astype(jnp.float32)
        chosen_sum = jnp.sum(probs * picked, axis=0, keepdims=True)
        combine = answers[:, 0, :]
        combine_ref[...] = combine
        mixed = jnp.sum(gates * combine, axis=0, keepdims=True)
        prob_grad = picked * (combine - mixed) / chosen_sum
        pairs = id_ref.shape[0] * tok_rows * 2 * LEVELS
        prob_grad = prob_grad + aux_ref[0] * (experts * answers[:, 1, :] / pairs)
        mean = jnp.sum(probs * prob_grad, axis=0, keepdims=True)
        logit_grad = probs * (prob_grad - mean)
        slope[...] = jnp.transpose(logit_grad).astype(jnp.bfloat16)
        part = token_ref.shape[1] // outbox.shape[0]

        @pl.loop(0, outbox.shape[0])
        def _(d):
            outbox[d] = jnp.dot(
                logit_grad.astype(jnp.bfloat16),
                token_ref[:, pl.ds(pl.multiple_of(d * part, part), part)],
                preferred_element_type=jnp.float32,
            ).astype(jnp.bfloat16)

    capacity = first_ref.shape[2]
    width = held.shape[-1]
    hidden = first_ref.shape[3]
    started = []

    def start(copy, when=None):
        if when is None:
            copy.start()
        else:
            pl.when(when)(copy.start)
        started.append((copy, when))

    def weight_copies(chunk):
        return [
            pltpu.make_async_copy(
                ref.at[pl.ds(chunk * width, width)],
                weights.at[chunk % 2, i],
                weight_sem.at[chunk, i],
            )
            for i, ref in enumerate((gate_ref, up_ref))
        ]

    def back_rows(chunk, core, store):
        group = 4

        @pl.loop(0, BLOCKS // group)
        def _(i):
            total = None
            for j, ref in enumerate((first_ref, second_ref)):
                term = lax.dot_general(
                    ref[core, pl.ds(i * group, group)].reshape(-1, hidden),
                    weights[chunk % 2, j],
                    (((1,), (1,)), ((), ())),
                    preferred_element_type=jnp.float32,
                )
                total = term if total is None else total + term
            store(i * group, group, total.astype(jnp.bfloat16).reshape(group, capacity, width))

    def leave(chunk):
        return sibling_copy(
            leaving.at[chunk % 2],
            held.at[chunk, :, pl.ds(capacity, capacity)],
            peer_send.at[chunk],
            peer_recv.at[chunk],
        )

    def step(chunk, name):
        kind, k = name
        z_first, swap = RETURN_TYPES[chunk]
        near = Copies(swap)
        p, q = near.p, near.q

        def give(block, slot, index, dz=None, dp=0, dq=0, when=None):
            start(
                near.remote(
                    held.at[chunk, block],
                    landed.at[chunk, slot],
                    send.at[chunk, index],
                    recv.at[chunk, slot],
                    z if dz is None else z + dz,
                    1 - p if dp else p,
                    1 - q if dq else q,
                ),
                when,
            )

        def take(block, slot):
            ref = landed.at[chunk, slot]
            near.remote(ref, ref, send.at[chunk, 0], recv.at[chunk, slot], z, 1 - p, q).wait_recv()
            held[chunk, block] = (
                held[chunk, block].astype(jnp.float32) + landed[chunk, slot].astype(jnp.float32)
            ).astype(jnp.bfloat16)

        def take_outer(block, level, base):
            pl.when(jnp.where(level > z, z > 0, z < LEVELS - 1))(lambda: take(block, base + level))

        def give_inner(block, level, base, index):
            up = level > z
            last = level == z - 1
            give(
                block,
                base + jnp.where(last, LEVELS, level),
                index,
                dz=jnp.where(up, 1, -1),
            )

        def take_ends(block, base):
            pl.when(z > 0)(lambda: take(block, base + z))
            pl.when(z < LEVELS - 1)(lambda: take(block, base + LEVELS))

        level = None if kind == "leaf" else nearest(z, k)
        if kind == "away":
            for copy in weight_copies(chunk):
                copy.wait()
            if chunk >= 2:
                leave(chunk - 2).wait_send()

            def store(at, count, value):
                leaving[chunk % 2, pl.ds(at, count)] = value

            back_rows(chunk, 1 - c, store)
            leave(chunk).start()
        elif kind == "near":

            def store(at, count, value):
                held[chunk, pl.ds(at, count), pl.ds(0, capacity)] = value

            back_rows(chunk, c, store)
            if chunk + 2 < CHUNKS:
                for copy in weight_copies(chunk + 2):
                    copy.start()
            leave(chunk).wait_recv()

            @pl.loop(0, BLOCKS, unroll=4)
            def _(b):
                held[chunk, b] = jnp.dot(
                    join_ref[b], held[chunk, b], preferred_element_type=jnp.float32
                ).astype(jnp.bfloat16)
        elif kind == "leaf":
            side, far = k
            level = nearest(z, far)
            column = 1 - p if side else p
            give(near.block(level, column, 1 - q), level * 2 + column, far * 2 + side, dq=1)
        elif kind == "P" and z_first:
            block = near.block(level, 1 - p, q)
            take(block, level * 2 + 1 - p)
            give(block, 8 + level, 8 + k, dp=1)
        elif kind == "P":
            block = near.block(z, 1 - p, q)
            take(block, z * 2 + 1 - p)
            take_ends(block, 13)
            give(block, 18, 14, dp=1)
        elif kind == "Z":
            block = near.block(level, p, q)
            take(block, level * 2 + p)
            if z_first:
                take(block, 8 + level)
                take_outer(block, level, 12)
                give_inner(block, level, 12, 11 + k)
            else:
                take_outer(block, level, 8)
                give_inner(block, level, 8, 7 + k)
        elif kind == "Y":
            block = near.block(level, 1 - p, q)
            take(block, level * 2 + 1 - p)
            take_outer(block, level, 13)
            give_inner(block, level, 13, 10 + k)
        elif kind == "own":
            block = near.block(z, p, q)
            take(block, z * 2 + p)
            if z_first:
                take(block, 8 + z)
                take_ends(block, 12)
            else:
                take_ends(block, 8)
                take(block, 18)
            here = slice(chunk * width, (chunk + 1) * width)
            routed = jnp.dot(slope[...], router_ref[:, here], preferred_element_type=jnp.float32)
            out_ref[:, here] = (held[chunk, block].astype(jnp.float32) + routed).astype(jnp.bfloat16)

    for chunk in range(2):
        for copy in weight_copies(chunk):
            copy.start()
    replies.post()
    begun = False
    for chunk, name in listed(RETURN_ORDER, return_names):
        step(chunk, name)
        if not begun:
            begun = True
            replies.collect()
            route_back()
            mail.post()
    mail.collect()
    total_ref[...] = jnp.sum(inbox[...].astype(jnp.float32), axis=0)
    replies.close()
    mail.close()
    for chunk in range(CHUNKS - 2, CHUNKS):
        leave(chunk).wait_send()
    for copy, when in started:
        if when is None:
            copy.wait_send()
        else:
            pl.when(when)(copy.wait_send)


def return_call(
    first, second, joined, gate_weight, up_weight, reply, probs, shares, ids, aux, tokens, router
):
    model_width, hidden = gate_weight.shape
    capacity = first.shape[2]
    rows = joined.shape[1]
    experts, devices = router.shape[0], reply.shape[0]
    width = model_width // CHUNKS
    dma = pltpu.SemaphoreType.DMA
    vmem, anywhere = pl.BlockSpec(memory_space=pltpu.VMEM), pl.BlockSpec(memory_space=pl.ANY)
    post = pltpu.VMEM((devices, experts, model_width // devices), jnp.bfloat16)
    return pl.pallas_call(
        return_kernel,
        out_shape=(
            jax.ShapeDtypeStruct((rows, model_width), jnp.bfloat16),
            jax.ShapeDtypeStruct((experts, rows), jnp.float32),
            jax.ShapeDtypeStruct((experts, model_width // devices), jnp.float32),
        ),
        in_specs=[vmem, vmem, vmem, anywhere, anywhere]
        + [vmem] * 4
        + [pl.BlockSpec(memory_space=pltpu.SMEM), vmem, vmem],
        out_specs=(vmem, vmem, vmem),
        scratch_shapes=[
            pltpu.VMEM((CHUNKS, BLOCKS, rows, width), jnp.bfloat16),
            pltpu.VMEM((CHUNKS, 19, rows, width), jnp.bfloat16),
            pltpu.VMEM((2, BLOCKS, capacity, width), jnp.bfloat16),
            pltpu.VMEM((2, 2, width, hidden), jnp.bfloat16),
            dma((CHUNKS, 2)),
            dma((CHUNKS, 15)),
            dma((CHUNKS, 19)),
            dma((CHUNKS,)),
            dma((CHUNKS,)),
            pltpu.VMEM(reply.shape, jnp.float32),
            pltpu.VMEM((rows, experts), jnp.bfloat16),
            post,
            post,
            dma((devices,)),
            dma((devices,)),
            dma((devices,)),
            dma((devices,)),
        ],
        compiler_params=pltpu.CompilerParams(
            has_side_effects=True, vmem_limit_bytes=60 * 2**20
        ),
        name="back_return",
    )(first, second, joined, gate_weight, up_weight, reply, probs, shares, ids, aux, tokens, router)


def gathered_shards(
    tokens,
    out_grad,
    router_weight,
    gate_weight,
    up_weight,
    down_weight,
    saved_gate,
    saved_up,
    expert_ids,
    aux_weight,
):
    inputs = tokens[0]
    chosen_ids = expert_ids[0]
    experts = router_weight.shape[1]
    router, ids = router_weight.T, chosen_ids.T

    grad_first, grad_second, joined, reply, router_probs, gate_dense = gather_call(
        out_grad[0], down_weight[0], inputs, router, ids, saved_gate[0], saved_up[0]
    )
    token_grad, combine_dense, router_grad = return_call(
        grad_first,
        grad_second,
        joined,
        gate_weight[0],
        up_weight[0],
        reply,
        router_probs,
        gate_dense,
        ids,
        aux_weight,
        inputs,
        router,
    )
    onehot = chosen_ids[:, None, :] == jnp.arange(experts, dtype=jnp.int32)[:, None]
    combine_grad = jnp.sum(jnp.where(onehot, combine_dense.T[:, :, None], 0.0), axis=1)
    return (token_grad[None], combine_grad[None], router_grad.T)


def program(*arrays):
    tok_rows = arrays[0].shape[1]
    seq_size, exp_size = lax.axis_size("seq"), lax.axis_size("exp")
    slots = arrays[6].shape[1]
    lined = exp_size == 4 and seq_size == 2 * LEVELS
    fits = arrays[0].shape[2] == 4096 and arrays[6].shape[2] == 768 and tok_rows == 128
    if lined and fits and seq_size * exp_size * tok_rows <= 2 * slots:
        return gathered_shards(*arrays)
    return shards(*arrays)


def solution(mesh):
    placed = (
        P("exp", "seq", None),
        P("exp", "seq", None),
        P(),
        P(("seq", "exp"), None, None),
        P(("seq", "exp"), None, None),
        P(("seq", "exp"), None, None),
        P(("seq", "exp"), None, None),
        P(("seq", "exp"), None, None),
        P("exp", "seq", None),
        P(),
    )
    return jax.shard_map(
        program,
        mesh=mesh,
        in_specs=placed,
        out_specs=(P("exp", "seq", None), P("exp", "seq", None), P(("seq", "exp"), None)),
        check_vma=False,
    )
```
